32 devices in a mesh: tile: 8 (over z, x), conv: 4 (over y, core).
Axes of the slice: x: 2, y: 2, z: 4, core: 2. Of those that a mesh axis runs over, the one named last changes fastest.
Arguments:
- field: float32 [256, 24576], P(None, ('tile', 'conv')), may hold values from -6 to 6
- interp: bfloat16 [32768, 384], P(('tile', 'conv')), may hold values from -0.1875 to 0.1875
- conv_blocks: bfloat16 [64, 3, 256, 256], P(('tile', 'conv')), may hold values from -0.21875 to 0.21875
- band_shift: int32 [64, 3], P(('tile', 'conv')), may hold values from 0 to 1
- owner: int32 [12288, 1], P(('tile', 'conv')), may hold values from 0 to 3; in each aligned block of 384 rows (0 to 383, 384 to 767, ...) at most 128 rows name the same one
- edge_index: int32 [64, 128], P(('tile', 'conv')), may hold values from 0 to 767, as said below
Outputs:
- correlated: float32 [256, 24576], P(None, ('tile', 'conv'))
The draws below stay inside these ranges and needn't reach their ends.
Inputs may be any that keep to these rules, and one draw needn't show every extreme that they name: `edge_index`: row 2b lists the first 128 columns of domain b in some order, row 2b + 1 its last 128 columns in some order. Among the 384 points of one domain no owner is named more than 128 times, and in some domains one owner is named exactly 128 times.
All inputs are finite; a program needn't handle non-finite values.
Results may differ from the reference program's by a relative error of at most 0.0049.
Values may be sent and summed in bfloat16 or wider, within the bound.
A program may use at most 64 MiB of HBM per device.

```python
import math
import jax
import jax.numpy as jnp
import numpy as np
from jax import lax

COLUMNS = 768
HALO_WIDTH = 128
BLOCK_POINTS = 256
OWNER_BLOCKS = 2
BAND_COUNT = 3
FIELD_ROWS = 256
DOMAINS = 32
ALL_COLUMNS = 24576
EXTENDED = 1024
SLOTS = 512
SUBPOINTS = 384
CAPACITY = 128
ALL_SUBPOINTS = 12288
N_TILE = 8
N_CONV = 4


def draw_edge_index(key, part):
    row_keys = jax.random.split(key, 2 * DOMAINS)
    orders = jax.vmap(lambda single: jax.random.permutation(single, HALO_WIDTH))(row_keys)
    side_flags = jnp.arange(2 * DOMAINS, dtype=jnp.int32) % 2
    offsets = side_flags * (COLUMNS - HALO_WIDTH)
    return (orders.astype(jnp.int32) + offsets[:, None]).astype(jnp.int32)


def with_ends(values, own_key, smallest, high):
    longest = values.shape.index(max(values.shape))
    spots = []
    for shift in (0, 1):
        where = [jax.random.randint(jax.random.fold_in(own_key, axis), (), 0, length) for axis, length in enumerate(values.shape)]
        where[longest] = (where[longest] + shift) % values.shape[longest]
        spots.append(tuple(where))
    return values.at[spots[0]].set(smallest).at[spots[1]].set(high)


def steps_of(key, shape, cuts, low, top_value):
    gain, own = 1.0, jax.random.fold_in(key, 6)
    for axis_at, shards_of in cuts:
        steps = jnp.exp(jax.random.uniform(jax.random.fold_in(own, axis_at), (shards_of,), jnp.float32, low / len(cuts), top_value / len(cuts)))
        gain = gain * jnp.repeat(steps, shape[axis_at] // shards_of).reshape([-1 if axis == axis_at else 1 for axis in range(len(shape))])
    return gain


def routed_block(own_key, own, number, rows, amount, top, limit, skew):
    sequence = jax.random.permutation(own_key, amount)
    crowded, ordinary = portions_of(amount, rows * top, limit, skew, True), portions_of(amount, rows * top, limit, skew, False)
    places = jnp.arange(amount)

    def named(sizes, rotation):
        used = int((sizes > 0).sum())
        fixed = max(1, used // 4)
        passed = fixed + (places - fixed + rotation * (used - fixed)) % max(1, amount - fixed)
        return jnp.zeros((amount,), jnp.int32).at[sequence[jnp.where(places < fixed, places, passed)]].set(jnp.asarray(sizes, jnp.int32))

    sizes = jnp.where(number % 4 == 0, named(crowded, number // 4), named(ordinary, number - number // 4 - 1))
    mixed = jax.random.permutation(jax.random.fold_in(own, 3), amount)
    source_of, taker = mixed[0:amount // 2 * 2:2], mixed[1:amount // 2 * 2:2]
    room = jnp.minimum(sizes[source_of] - 1, limit - sizes[taker]) // 2
    room = jnp.where((source_of == sequence[0]) | (taker == sequence[0]) | (sizes[taker] == 0), 0, jnp.maximum(room, 0))
    passed = jax.random.randint(jax.random.fold_in(own, 4), (amount // 2,), 0, 1 << 20) % (room + 1)
    sizes = sizes.at[source_of].add(-passed).at[taker].add(passed)
    members = jnp.searchsorted(jnp.cumsum(sizes), jnp.arange(rows * top), side="right").astype(jnp.int32)
    listing = members.reshape(top, rows).T
    listing = listing[jax.random.permutation(jax.random.fold_in(own, 1), rows)]
    rotation = jax.random.randint(jax.random.fold_in(own, 2), (rows, 1), 0, top)
    return jnp.take_along_axis(listing, (jnp.arange(top)[None, :] + rotation) % top, axis=1)


def portions_of(count, total, reach, slope, full):
    loads = [(1 << 20) // math.isqrt(grade ** slope) + 1 for grade in range(1, count + 1)]
    largest = reach if full else min(reach, max(-(-total // count), total * loads[0] // sum(loads)))
    least = 1 if total - largest >= count - 1 else 0
    holding, surplus = [largest] + [least] * (count - 1), total - largest - least * (count - 1)
    while surplus > 0:
        movable = [i for i in range(1, count) if holding[i] < largest] or [i for i in range(1, count) if holding[i] < reach]
        mass, remaining = sum([loads[i] for i in movable]), surplus
        for i in movable:
            addition = min(reach - holding[i], max(1, remaining * loads[i] // mass), surplus)
            holding[i] = holding[i] + addition
            surplus = surplus - addition
    return np.array(holding)


def gaussian(stream_key, dims, width, limit, cuts=(), kind=jnp.bfloat16):
    drawn = width * jax.random.normal(stream_key, dims, jnp.float32)
    if cuts:
        drawn = drawn * steps_of(stream_key, dims, cuts, -0.22, 0.18)
    return jnp.clip(drawn, -limit, limit).astype(kind)


def setup_inputs(seed: int = 0) -> dict:
    streams_of = jax.random.split(jax.random.key(seed), 7)
    field = gaussian(streams_of[0], (FIELD_ROWS, ALL_COLUMNS), 1.0, 6.0, ((1, 32),), jnp.float32)
    interp = gaussian(streams_of[1], (DOMAINS * EXTENDED, SUBPOINTS), EXTENDED ** -0.5, 0.1875, ((0, 32),))
    conv_blocks = gaussian(streams_of[2], (DOMAINS * OWNER_BLOCKS, BAND_COUNT, BLOCK_POINTS, BLOCK_POINTS), (BAND_COUNT * BLOCK_POINTS) ** -0.5, 0.21875, ((0, 32),))
    band_shift = with_ends(jax.random.randint(streams_of[3], (DOMAINS * OWNER_BLOCKS, BAND_COUNT), 0, OWNER_BLOCKS), jax.random.fold_in(streams_of[3], 1), 0, OWNER_BLOCKS - 1).astype(jnp.int32)
    owner_keys = jax.random.split(jax.random.fold_in(streams_of[4], 1), ALL_SUBPOINTS // SUBPOINTS)
    owner_turns = jax.random.permutation(jax.random.fold_in(streams_of[4], 3), ALL_SUBPOINTS // SUBPOINTS)
    owner = jax.vmap(lambda own, number: routed_block(jax.random.fold_in(streams_of[4], 2), own, number, SUBPOINTS, N_CONV, 1, CAPACITY, 2))(owner_keys, owner_turns).reshape((ALL_SUBPOINTS, 1))
    edge_index = draw_edge_index(jax.random.fold_in(streams_of[6], 71), 0)
    return dict(field=field, interp=interp, conv_blocks=conv_blocks, band_shift=band_shift, owner=owner, edge_index=edge_index)


def slot_table(owners):
    choose = (owners[:, None] == jnp.arange(N_CONV, dtype=jnp.int32)[None, :]).astype(jnp.int32)
    before = jnp.cumsum(choose, axis=0) - choose
    position = jnp.sum(before * choose, axis=1)
    slot_index = owners * CAPACITY + position
    return (slot_index[:, None] == jnp.arange(SLOTS, dtype=jnp.int32)[None, :]).astype(jnp.float32)


def interpolate(operands):
    extended, weights, owners = operands
    subgrid = jnp.dot(extended, weights, preferred_element_type=jnp.float32).astype(jnp.bfloat16)
    packed = jnp.dot(subgrid.astype(jnp.float32), slot_table(owners), precision=lax.Precision.HIGHEST)
    return packed.astype(jnp.bfloat16)


def convolve(operands):
    values, blocks, shifts = operands
    height = values.shape[0]
    pieces = values.reshape(height, OWNER_BLOCKS, BLOCK_POINTS).astype(jnp.float32)
    source = (jnp.arange(OWNER_BLOCKS, dtype=jnp.int32)[:, None] + shifts) % OWNER_BLOCKS
    picked = pieces[:, source, :]
    matrices = blocks.astype(jnp.float32)
    forward = jnp.einsum("rjbp,jbpq->rjq", picked, matrices, precision=lax.Precision.HIGHEST).astype(jnp.bfloat16)
    backward = jnp.einsum("rjq,jbpq->rjbp", forward.astype(jnp.float32), matrices, precision=lax.Precision.HIGHEST)
    select = (source[:, :, None] == jnp.arange(OWNER_BLOCKS, dtype=jnp.int32)[None, None, :]).astype(jnp.float32)
    adjoint = jnp.einsum("rjbp,jbs->rsp", backward, select, precision=lax.Precision.HIGHEST)
    return adjoint.reshape(height, SLOTS).astype(jnp.bfloat16)


def adjoint_interpolate(operands):
    returned_slots, weights, owners = operands
    returned = jnp.dot(returned_slots.astype(jnp.float32), slot_table(owners).T, precision=lax.Precision.HIGHEST)
    returned = returned.astype(jnp.bfloat16)
    return jnp.dot(returned, weights.T, preferred_element_type=jnp.float32)


def add_edges(inner_part, left_sum, right_sum, left_list, right_list):
    inner_part = inner_part.at[:, left_list].add(left_sum)
    return inner_part.at[:, right_list].add(right_sum)


def reference(field, interp, conv_blocks, band_shift, owner, edge_index):
    field_rows = field.shape[0]
    rounded = field.astype(jnp.bfloat16).reshape(field_rows, DOMAINS, COLUMNS).transpose(1, 0, 2)
    edges = edge_index.reshape(DOMAINS, 2, HALO_WIDTH)
    left_lists = edges[:, 0, :]
    right_lists = edges[:, 1, :]
    left_index = jnp.broadcast_to(left_lists[:, None, :], (DOMAINS, field_rows, HALO_WIDTH))
    right_index = jnp.broadcast_to(right_lists[:, None, :], (DOMAINS, field_rows, HALO_WIDTH))
    left_values = jnp.take_along_axis(rounded, left_index, axis=2)
    right_values = jnp.take_along_axis(rounded, right_index, axis=2)
    extended = jnp.concatenate([jnp.roll(right_values, 1, axis=0), rounded, jnp.roll(left_values, -1, axis=0)], axis=2)
    weights = interp.reshape(DOMAINS, EXTENDED, SUBPOINTS)
    owners = owner.reshape(DOMAINS, SUBPOINTS)
    packed = lax.map(interpolate, (extended, weights, owners))
    gathered = packed.reshape(N_TILE, N_CONV, field_rows, N_CONV, CAPACITY).transpose(0, 3, 2, 1, 4)
    gathered = gathered.reshape(DOMAINS, field_rows, SLOTS)
    blocks = conv_blocks.reshape(DOMAINS, OWNER_BLOCKS, BAND_COUNT, BLOCK_POINTS, BLOCK_POINTS)
    shifts = band_shift.reshape(DOMAINS, OWNER_BLOCKS, BAND_COUNT)
    adjoints = lax.map(convolve, (gathered, blocks, shifts))
    returned = adjoints.reshape(N_TILE, N_CONV, field_rows, N_CONV, CAPACITY).transpose(0, 3, 2, 1, 4)
    returned = returned.reshape(DOMAINS, field_rows, SLOTS)
    partial_value = lax.map(adjoint_interpolate, (returned, weights, owners))
    interior = partial_value[:, :, HALO_WIDTH:HALO_WIDTH + COLUMNS]
    left_sums = jnp.roll(partial_value[:, :, HALO_WIDTH + COLUMNS:], 1, axis=0)
    right_sums = jnp.roll(partial_value[:, :, :HALO_WIDTH], -1, axis=0)
    result = jax.vmap(add_edges)(interior, left_sums, right_sums, left_lists, right_lists)
    return result.transpose(1, 0, 2).reshape(field_rows, DOMAINS * COLUMNS)
```

```python
import functools

import jax
import jax.numpy as jnp
from jax import lax
from jax.experimental import pallas as pl
from jax.experimental.pallas import tpu as pltpu
from jax.sharding import PartitionSpec as P

MESH = pl.DeviceIdType.MESH
CHUNKS = 2


def mm(left, right):
    return lax.dot_general(left, right, (((1,), (0,)), ((), ())), preferred_element_type=jnp.float32)


def mm_t(left, right):
    return lax.dot_general(left, right, (((1,), (1,)), ((), ())), preferred_element_type=jnp.float32)


def kernel(
    tiles, groups, rim, field_hbm, interp_hbm, blocks_hbm, owner_hbm, index_hbm, shift_hbm, result,
    field, interp, blocks, owner, index, shift, ip, conv, gram, base,
    edge_out, edge_in, late_in, rim_out, rim_in, cell_out, slot_in, back_in, far_out, far_in, part_out, part_in,
    load_sem, send_sem, edge_recv, late_recv, rim_recv, slot_recv, back_recv, part_recv,
):
    rows, columns = field.shape
    extended, points = interp.shape
    owned, bands, size = blocks.shape[0], blocks.shape[1], blocks.shape[2]
    slots = owned * size
    capacity = slots // groups
    height = rows // CHUNKS
    last = groups - 1
    tile, me = lax.axis_index("tile"), lax.axis_index("conv")
    after, before = lax.rem(tile + 1, tiles), lax.rem(tile + tiles - 1, tiles)
    up, down = lax.rem(me + 1, groups), lax.rem(me + last, groups)
    hops = [groups // 2] + [k for k in range(1, groups) if k != groups // 2]
    peers = [lax.rem(me + k, groups) for k in hops]

    barrier = pltpu.get_barrier_semaphore()

    def greet(target):
        pl.semaphore_signal(barrier, inc=1, device_id=target, device_id_type=MESH)

    greet((before, last))
    greet((after, 0))

    @pl.when(me == 0)
    def _():
        for g in range(last):
            greet((before, g))

    @pl.when(me == last)
    def _():
        for g in range(1, groups):
            greet((after, g))

    for peer in peers:
        greet((tile, peer))

    def load(source, target, at):
        copy = pltpu.make_async_copy(source, target, load_sem.at[at])
        copy.start()
        return copy

    def drain(ref, semaphore):
        pltpu.make_async_copy(ref, ref, semaphore).wait()

    inner = slice(rim, columns - rim)
    lead, tail = slice(0, rim), slice(columns - rim, columns)
    load_index = load(index_hbm, index, 0)
    load_lead = load(field_hbm.at[:, lead], field.at[:, lead], 1)
    load_tail = load(field_hbm.at[:, tail], field.at[:, tail], 2)
    load_owner = load(owner_hbm, owner, 3)
    load_interp = load(interp_hbm, interp, 4)
    load_inner = load(field_hbm.at[:, inner], field.at[:, inner], 5)
    load_shift = load(shift_hbm, shift, 6)
    load_blocks = load(blocks_hbm, blocks, 7)

    def piece(chunk):
        return slice(chunk * height, (chunk + 1) * height)

    def send(source, target, kind, arrival, place):
        pltpu.make_async_remote_copy(
            src_ref=source, dst_ref=target, send_sem=send_sem.at[kind], recv_sem=arrival,
            device_id=place, device_id_type=MESH,
        ).start()

    def exchange(kind, chunk, in_ref, recv):
        for peer in peers:
            send(cell_out.at[kind, chunk, peer], in_ref.at[chunk, me], 0, recv.at[chunk], (tile, peer))
        in_ref[chunk, me] = cell_out[kind, chunk, me]

    def arrived(chunk, in_ref, recv):
        drain(in_ref.at[chunk, 0:last], recv.at[chunk])
        return [in_ref[chunk, g] for g in range(groups)]

    load_index.wait()
    left_list, right_list = index[0:1, :], index[1:2, :]
    lines = lax.broadcasted_iota(jnp.int32, (rim, rim), 0)
    left_pick = (lines == left_list).astype(jnp.float32).astype(jnp.bfloat16)
    right_pick = (lines + (columns - rim) == right_list).astype(jnp.float32).astype(jnp.bfloat16)
    load_lead.wait()
    load_tail.wait()
    for chunk in range(CHUNKS):
        part = piece(chunk)
        edge_out[chunk, 0] = mm(field[part, tail].astype(jnp.bfloat16), right_pick).astype(jnp.bfloat16)
        edge_out[chunk, 1] = mm(field[part, lead].astype(jnp.bfloat16), left_pick).astype(jnp.bfloat16)

    load_owner.wait()
    owners = owner[...]
    choose = (owners == lax.broadcasted_iota(jnp.int32, (-(-groups // 8) * 8, points), 0)).astype(jnp.float32)
    order = lax.broadcasted_iota(jnp.int32, (points, points), 0) < lax.broadcasted_iota(
        jnp.int32, (points, points), 1
    )
    ranks = mm(choose.astype(jnp.bfloat16), order.astype(jnp.float32).astype(jnp.bfloat16))
    rank = jnp.sum(ranks * choose, axis=0, keepdims=True)
    slot = owners * capacity + rank.astype(jnp.int32)
    placement = (slot == lax.broadcasted_iota(jnp.int32, (slots, points), 0)).astype(jnp.float32)
    placement = placement.astype(jnp.bfloat16)
    load_interp.wait()
    ip[0:rim, :] = mm_t(interp[0:rim, :], placement).astype(jnp.bfloat16)
    ip[rim : 2 * rim, :] = mm_t(interp[extended - rim :, :], placement).astype(jnp.bfloat16)

    def share(side, at):
        for g in range(groups):
            rim_out[g] = ip[side * rim : (side + 1) * rim, g * capacity : (g + 1) * capacity]
        rim_in[side] = rim_out[at]
        for chunk in range(CHUNKS):
            edge_in[chunk, side] = jnp.zeros((height, rim), jnp.bfloat16)

    pl.when(me == 0)(functools.partial(share, 0, 0))
    pl.when(me == last)(functools.partial(share, 1, last))

    pl.semaphore_wait(barrier, jnp.where((me == 0) | (me == last), 2 * groups, last + 2))

    for chunk in range(CHUNKS):

        @pl.when(me == 0)
        def _():
            for g in range(groups):
                send(edge_out.at[chunk, 1], late_in.at[chunk, 1], 1, late_recv.at[chunk], (before, g))

        @pl.when(me == last)
        def _():
            for g in range(groups):
                send(edge_out.at[chunk, 0], late_in.at[chunk, 0], 1, late_recv.at[chunk], (after, g))

        @pl.when(me < last)
        def _():
            send(edge_out.at[chunk, 0], edge_in.at[chunk, 0], 2, edge_recv.at[chunk, 0], (tile, up))

        @pl.when(me > 0)
        def _():
            send(edge_out.at[chunk, 1], edge_in.at[chunk, 1], 2, edge_recv.at[chunk, 1], (tile, down))

    @pl.when(me == 0)
    def _():
        for g in range(1, groups):
            send(rim_out.at[g], rim_in.at[0], 3, rim_recv.at[0], (tile, g))

    @pl.when(me == last)
    def _():
        for g in range(last):
            send(rim_out.at[g], rim_in.at[1], 3, rim_recv.at[1], (tile, g))

    ip[2 * rim :, :] = mm_t(interp[rim : extended - rim, :], placement).astype(jnp.bfloat16)
    load_inner.wait()
    base[...] = mm(field[...].astype(jnp.bfloat16), ip[2 * rim :, :])

    load_shift.wait()
    load_blocks.wait()
    for j in range(owned):
        for s in range(owned):
            total = jnp.zeros((size, size), jnp.float32)
            for c in range(bands):
                reads = lax.rem(j + shift[j : j + 1, c : c + 1], owned) == s
                total = total + jnp.where(reads, 1.0, 0.0) * blocks[j, c].astype(jnp.float32)
            conv[s * size : (s + 1) * size, j * size : (j + 1) * size] = total.astype(jnp.bfloat16)
    gram[...] = mm_t(conv[...], conv[...]).astype(jnp.bfloat16)

    for chunk in range(CHUNKS):
        pl.when(me > 0)(lambda: drain(edge_in.at[chunk, 0], edge_recv.at[chunk, 0]))
        pl.when(me < last)(lambda: drain(edge_in.at[chunk, 1], edge_recv.at[chunk, 1]))
        edges = jnp.concatenate([edge_in[chunk, 0], edge_in[chunk, 1]], axis=1)
        subgrid = (base[piece(chunk), :] + mm(edges, ip[0 : 2 * rim, :])).astype(jnp.bfloat16)
        for g in range(groups):
            cell_out[0, chunk, g] = subgrid[:, g * capacity : (g + 1) * capacity]
        exchange(0, chunk, slot_in, slot_recv)

    pl.when(me > 0)(lambda: drain(rim_in.at[0], rim_recv.at[0]))
    pl.when(me < last)(lambda: drain(rim_in.at[1], rim_recv.at[1]))
    for chunk in range(CHUNKS):
        cells = arrived(chunk, slot_in, slot_recv)
        drain(late_in.at[chunk], late_recv.at[chunk])
        for side, g in ((0, 0), (1, last)):
            cells[g] = (cells[g].astype(jnp.float32) + mm(late_in[chunk, side], rim_in[side])).astype(jnp.bfloat16)
        adjoint = mm(jnp.concatenate(cells, axis=1), gram[...]).astype(jnp.bfloat16)
        for g in range(groups):
            cell_out[1, chunk, g] = adjoint[:, g * capacity : (g + 1) * capacity]
        exchange(1, chunk, back_in, back_recv)
        for side, g in ((0, 0), (1, last)):
            far_out[chunk, side] = mm_t(cell_out[1, chunk, g], rim_in[side]).astype(jnp.bfloat16)
        send(far_out.at[chunk, 0], far_in.at[chunk, me], 4, part_recv.at[chunk, 1], (before, last))
        send(far_out.at[chunk, 1], far_in.at[chunk, me], 4, part_recv.at[chunk, 0], (after, 0))

    for chunk in range(CHUNKS):
        part = piece(chunk)
        returned = jnp.concatenate(arrived(chunk, back_in, back_recv), axis=1)
        rims = mm_t(returned, ip[0 : 2 * rim, :]).astype(jnp.bfloat16)
        part_out[chunk, 0] = rims[:, rim:]
        part_out[chunk, 1] = rims[:, :rim]

        @pl.when(me < last)
        def _():
            send(part_out.at[chunk, 0], part_in.at[chunk, 0], 5, part_recv.at[chunk, 0], (tile, up))

        @pl.when(me > 0)
        def _():
            send(part_out.at[chunk, 1], part_in.at[chunk, 1], 5, part_recv.at[chunk, 1], (tile, down))

        result[part, :] = mm_t(returned, ip[2 * rim :, :])

    for chunk in range(CHUNKS):
        part = piece(chunk)
        for side, where, pick, end in ((0, lead, left_pick, 0), (1, tail, right_pick, last)):

            @pl.when(me != end)
            def _():
                drain(part_in.at[chunk, side], part_recv.at[chunk, side])
                result[part, where] += mm_t(part_in[chunk, side], pick)

            @pl.when(me == end)
            def _():
                drain(far_in.at[chunk], part_recv.at[chunk, side])
                total = result[part, where]
                for g in range(groups):
                    total = total + mm_t(far_in[chunk, g], pick)
                result[part, where] = total

    drain(cell_out.at[:, :, 0:last], send_sem.at[0])
    drain(far_out, send_sem.at[4])

    @pl.when((me == 0) | (me == last))
    def _():
        drain(far_in, send_sem.at[1])
        drain(edge_out.at[:, 0], send_sem.at[2])
        drain(rim_out.at[0:last], send_sem.at[3])
        drain(part_out.at[:, 0], send_sem.at[5])

    @pl.when((me != 0) & (me != last))
    def _():
        drain(edge_out, send_sem.at[2])
        drain(part_out, send_sem.at[5])


def in_hbm(array):
    return pltpu.with_memory_space_constraint(array, pltpu.HBM)


def on_device(tiles, groups, field, interp, conv_blocks, band_shift, owner, edge_index):
    rows, columns = field.shape
    extended, points = interp.shape
    rim = edge_index.shape[1]
    slots = conv_blocks.shape[0] * conv_blocks.shape[2]
    capacity = slots // groups
    height = rows // CHUNKS
    half, single = jnp.bfloat16, jnp.float32
    sides = pltpu.VMEM((CHUNKS, 2, height, rim), half)
    cells = pltpu.VMEM((CHUNKS, groups, height, capacity), half)
    dma = pltpu.SemaphoreType.DMA
    anywhere = pl.BlockSpec(memory_space=pltpu.HBM)
    return pl.pallas_call(
        functools.partial(kernel, tiles, groups, rim),
        out_shape=jax.ShapeDtypeStruct(field.shape, single),
        in_specs=[anywhere] * 6,
        out_specs=pl.BlockSpec(memory_space=pltpu.VMEM),
        scratch_shapes=[
            pltpu.VMEM(field.shape, single),
            pltpu.VMEM(interp.shape, half),
            pltpu.VMEM(conv_blocks.shape, half),
            pltpu.VMEM((1, points), jnp.int32),
            pltpu.VMEM(edge_index.shape, jnp.int32),
            pltpu.VMEM(band_shift.shape, jnp.int32),
            pltpu.VMEM((extended, slots), half),
            pltpu.VMEM((slots, slots), half),
            pltpu.VMEM((slots, slots), half),
            pltpu.VMEM((rows, slots), single),
            sides, sides, sides,
            pltpu.VMEM((groups, rim, capacity), half),
            pltpu.VMEM((2, rim, capacity), half),
            pltpu.VMEM((2, CHUNKS, groups, height, capacity), half),
            cells, cells,
            sides,
            pltpu.VMEM((CHUNKS, groups, height, rim), half),
            sides, sides,
            dma((8,)), dma((6,)), dma((CHUNKS, 2)), dma((CHUNKS,)), dma((2,)), dma((CHUNKS,)), dma((CHUNKS,)),
            dma((CHUNKS, 2)),
        ],
        compiler_params=pltpu.CompilerParams(collective_id=0, has_side_effects=True, vmem_limit_bytes=53 * 2**20),
    )(field, interp, conv_blocks, *[in_hbm(small) for small in (owner.reshape(1, -1), edge_index, band_shift)])


def solution(mesh):
    return jax.shard_map(
        functools.partial(on_device, mesh.shape["tile"], mesh.shape["conv"]),
        mesh=mesh,
        in_specs=(
            P(None, ("tile", "conv")),
            P(("tile", "conv"), None),
            P(("tile", "conv"), None, None, None),
            P(("tile", "conv"), None),
            P(("tile", "conv"), None),
            P(("tile", "conv"), None),
        ),
        out_specs=P(None, ("tile", "conv")),
        check_vma=False,
    )
```

```python
import functools

import jax
import jax.numpy as jnp
from jax import lax
from jax.experimental import pallas as pl
from jax.experimental.pallas import tpu as pltpu
from jax.sharding import PartitionSpec as P

MESH = pl.DeviceIdType.MESH
CHUNKS = 2


def mm(left, right):
    return lax.dot_general(left, right, (((1,), (0,)), ((), ())), preferred_element_type=jnp.float32)


def mm_t(left, right):
    return lax.dot_general(left, right, (((1,), (1,)), ((), ())), preferred_element_type=jnp.float32)


def kernel(
    tiles, groups, rim, field_hbm, interp_hbm, blocks_hbm, owner_hbm, index_hbm, shift_hbm, result,
    field, interp, blocks, owner, index, shift, ip, conv, gram, base,
    edge_out, edge_in, relay, late_in, rim_out, rim_in, cell_out, slot_in, back_in, share, share_out, share_in, far_out, far_in, part_out, part_in,
    ready, load_sem, send_sem, edge_recv, relay_recv, late_recv, rim_recv, slot_recv, back_recv, share_recv, part_recv,
):
    rows, columns = field.shape
    extended, points = interp.shape
    owned, bands, size = blocks.shape[0], blocks.shape[1], blocks.shape[2]
    slots = owned * size
    capacity = slots // groups
    height = rows // CHUNKS
    last = groups - 1
    tile, me = lax.axis_index("tile"), lax.axis_index("conv")
    after, before = lax.rem(tile + 1, tiles), lax.rem(tile + tiles - 1, tiles)
    up, down = lax.rem(me + 1, groups), lax.rem(me + last, groups)
    hops = [groups // 2] + [k for k in range(1, groups) if k != groups // 2]
    peers = [lax.rem(me + k, groups) for k in hops]

    barrier = pltpu.get_barrier_semaphore()
    first_tile, last_tile = tile == 0, tile == tiles - 1
    odd = lax.rem(me, 2)
    even = odd == 0
    mate = me + 1 - 2 * odd

    def meet(lower, upper):
        return (upper == 0) | (lower == last) | (upper == lower - lax.rem(lower, 2))

    with_before = [meet(g, me) for g in range(groups)]
    with_after = [meet(me, g) for g in range(groups)]
    from_before = sum(jnp.where(met, 1, 0) for met in with_before)
    from_after = sum(jnp.where(met, 1, 0) for met in with_after)

    def signal(semaphore, target):
        pl.semaphore_signal(semaphore, inc=1, device_id=target, device_id_type=MESH)

    def tell(semaphore, there, met):
        for g in range(groups):
            pl.when(met[g])(functools.partial(signal, semaphore, (there, g)))

    def tell_before(semaphore):
        tell(semaphore, before, with_before)

    def tell_after(semaphore):
        tell(semaphore, after, with_after)

    pl.when(first_tile)(lambda: tell_before(barrier))
    pl.when(~last_tile)(lambda: tell_after(barrier))
    for peer in peers:
        signal(barrier, (tile, peer))

    def load(source, target, at):
        copy = pltpu.make_async_copy(source, target, load_sem.at[at])
        copy.start()
        return copy

    def drain(ref, semaphore):
        pltpu.make_async_copy(ref, ref, semaphore).wait()

    inner = slice(rim, columns - rim)
    lead, tail = slice(0, rim), slice(columns - rim, columns)
    load_index = load(index_hbm, index, 0)
    load_lead = load(field_hbm.at[:, lead], field.at[:, lead], 1)
    load_tail = load(field_hbm.at[:, tail], field.at[:, tail], 2)
    load_owner = load(owner_hbm, owner, 3)
    load_interp = load(interp_hbm, interp, 4)
    load_inner = load(field_hbm.at[:, inner], field.at[:, inner], 5)
    load_shift = load(shift_hbm, shift, 6)
    load_blocks = load(blocks_hbm, blocks, 7)

    def piece(chunk):
        return slice(chunk * height, (chunk + 1) * height)

    def send(source, target, kind, arrival, place):
        pltpu.make_async_remote_copy(
            src_ref=source, dst_ref=target, send_sem=send_sem.at[kind], recv_sem=arrival,
            device_id=place, device_id_type=MESH,
        ).start()

    def exchange(kind, chunk, in_ref, recv):
        for peer in peers:
            send(cell_out.at[kind, chunk, peer], in_ref.at[chunk, me], 0, recv.at[chunk], (tile, peer))
        in_ref[chunk, me] = cell_out[kind, chunk, me]

    def arrived(chunk, in_ref, recv):
        drain(in_ref.at[chunk, 0:last], recv.at[chunk])
        return [in_ref[chunk, g] for g in range(groups)]

    pl.semaphore_wait(
        barrier, last + jnp.where(first_tile, 0, from_before) + jnp.where(last_tile, from_after, 0)
    )
    pl.when(~first_tile)(lambda: tell_before(ready.at[1]))
    pl.when(last_tile)(lambda: tell_after(ready.at[0]))

    load_index.wait()
    left_list, right_list = index[0:1, :], index[1:2, :]
    lines = lax.broadcasted_iota(jnp.int32, (rim, rim), 0)
    left_pick = (lines == left_list).astype(jnp.float32).astype(jnp.bfloat16)
    right_pick = (lines + (columns - rim) == right_list).astype(jnp.float32).astype(jnp.bfloat16)
    load_lead.wait()
    load_tail.wait()
    for chunk in range(CHUNKS):
        part = piece(chunk)
        edge_out[chunk, 0] = mm(field[part, tail].astype(jnp.bfloat16), right_pick).astype(jnp.bfloat16)
        edge_out[chunk, 1] = mm(field[part, lead].astype(jnp.bfloat16), left_pick).astype(jnp.bfloat16)

    for chunk in range(CHUNKS):

        @pl.when(me < last)
        def _():
            send(edge_out.at[chunk, 0], edge_in.at[chunk, 0], 2, edge_recv.at[chunk, 0], (tile, up))

        @pl.when(me > 0)
        def _():
            send(edge_out.at[chunk, 1], edge_in.at[chunk, 1], 2, edge_recv.at[chunk, 1], (tile, down))

    @pl.when(me == 0)
    def _():
        relay[...] = edge_out[:, 1]
        for g in range(2, groups, 2):
            send(edge_out.at[:, 1], relay, 6, relay_recv.at[0], (tile, g))

    def late_right():
        for chunk in range(CHUNKS):
            for g in range(1, groups, 2):
                send(edge_out.at[chunk, 0], late_in.at[chunk, 0], 1, late_recv.at[chunk, 0], (after, g))

    pl.when((me == last) & last_tile)(late_right)

    load_owner.wait()
    owners = owner[...]
    choose = (owners == lax.broadcasted_iota(jnp.int32, (-(-groups // 8) * 8, points), 0)).astype(jnp.float32)
    order = lax.broadcasted_iota(jnp.int32, (points, points), 0) < lax.broadcasted_iota(
        jnp.int32, (points, points), 1
    )
    ranks = mm(choose.astype(jnp.bfloat16), order.astype(jnp.float32).astype(jnp.bfloat16))
    rank = jnp.sum(ranks * choose, axis=0, keepdims=True)
    slot = owners * capacity + rank.astype(jnp.int32)
    placement = (slot == lax.broadcasted_iota(jnp.int32, (slots, points), 0)).astype(jnp.float32)
    placement = placement.astype(jnp.bfloat16)
    load_interp.wait()
    ip[0:rim, :] = mm_t(interp[0:rim, :], placement).astype(jnp.bfloat16)
    ip[rim : 2 * rim, :] = mm_t(interp[extended - rim :, :], placement).astype(jnp.bfloat16)

    def spread(side, at):
        for g in range(groups):
            rim_out[g] = ip[side * rim : (side + 1) * rim, g * capacity : (g + 1) * capacity]
        rim_in[side] = rim_out[at]
        for chunk in range(CHUNKS):
            edge_in[chunk, side] = jnp.zeros((height, rim), jnp.bfloat16)

    pl.when(me == 0)(functools.partial(spread, 0, 0))
    pl.when(me == last)(functools.partial(spread, 1, last))

    @pl.when(me == 0)
    def _():
        for g in range(1, groups):
            send(rim_out.at[g], rim_in.at[0], 3, rim_recv.at[0], (tile, g))

    @pl.when(me == last)
    def _():
        for g in range(last):
            send(rim_out.at[g], rim_in.at[1], 3, rim_recv.at[1], (tile, g))

    ip[2 * rim :, :] = mm_t(interp[rim : extended - rim, :], placement).astype(jnp.bfloat16)
    load_inner.wait()
    base[...] = mm(field[...].astype(jnp.bfloat16), ip[2 * rim :, :])

    for chunk in range(CHUNKS):
        pl.when(me > 0)(lambda: drain(edge_in.at[chunk, 0], edge_recv.at[chunk, 0]))
        pl.when(me < last)(lambda: drain(edge_in.at[chunk, 1], edge_recv.at[chunk, 1]))
        edges = jnp.concatenate([edge_in[chunk, 0], edge_in[chunk, 1]], axis=1)
        subgrid = (base[piece(chunk), :] + mm(edges, ip[0 : 2 * rim, :])).astype(jnp.bfloat16)
        for g in range(groups):
            cell_out[0, chunk, g] = subgrid[:, g * capacity : (g + 1) * capacity]
        exchange(0, chunk, slot_in, slot_recv)

    @pl.when((me == last) & ~last_tile)
    def _():
        pl.semaphore_wait(ready.at[1], from_after)
        late_right()

    pl.when(even & (me != 0))(lambda: drain(relay, relay_recv.at[0]))

    @pl.when(even)
    def _():
        pl.when(first_tile)(lambda: pl.semaphore_wait(ready.at[0], from_before))
        for chunk in range(CHUNKS):
            for g in (me, me + 1):
                send(relay.at[chunk], late_in.at[chunk, 1], 1, late_recv.at[chunk, 1], (before, g))

    load_shift.wait()
    load_blocks.wait()
    for j in range(owned):
        for s in range(owned):
            total = jnp.zeros((size, size), jnp.float32)
            for c in range(bands):
                reads = lax.rem(j + shift[j : j + 1, c : c + 1], owned) == s
                total = total + jnp.where(reads, 1.0, 0.0) * blocks[j, c].astype(jnp.float32)
            conv[s * size : (s + 1) * size, j * size : (j + 1) * size] = total.astype(jnp.bfloat16)
    gram[...] = mm_t(conv[...], conv[...]).astype(jnp.bfloat16)

    pl.when(me > 0)(lambda: drain(rim_in.at[0], rim_recv.at[0]))
    pl.when(me < last)(lambda: drain(rim_in.at[1], rim_recv.at[1]))
    pl.when(~even & first_tile)(lambda: pl.semaphore_wait(ready.at[0], from_before))
    pl.when((me != last) & ~last_tile)(lambda: pl.semaphore_wait(ready.at[1], from_after))

    @pl.when(~even)
    def _():
        for chunk in range(CHUNKS):
            drain(late_in.at[chunk, 0], late_recv.at[chunk, 0])
            send(late_in.at[chunk, 0], late_in.at[chunk, 0], 8, late_recv.at[chunk, 0], (tile, mate))

    for chunk in range(CHUNKS):
        cells = arrived(chunk, slot_in, slot_recv)
        pl.when(even)(lambda: drain(late_in.at[chunk, 0], late_recv.at[chunk, 0]))
        drain(late_in.at[chunk, 1], late_recv.at[chunk, 1])
        for side, g in ((0, 0), (1, last)):
            cells[g] = (cells[g].astype(jnp.float32) + mm(late_in[chunk, side], rim_in[side])).astype(jnp.bfloat16)
        adjoint = mm(jnp.concatenate(cells, axis=1), gram[...]).astype(jnp.bfloat16)
        for g in range(groups):
            cell_out[1, chunk, g] = adjoint[:, g * capacity : (g + 1) * capacity]
        exchange(1, chunk, back_in, back_recv)
        share_out[chunk] = mm_t(cell_out[1, chunk, (1 - odd) * last], rim_in[1 - odd]).astype(jnp.bfloat16)
        send(share_out.at[chunk], share_in.at[chunk], 7, share_recv.at[chunk], (tile, mate))
        share[chunk] = mm_t(cell_out[1, chunk, odd * last], rim_in[odd])

    for chunk in range(CHUNKS):
        drain(share_in.at[chunk], share_recv.at[chunk])
        far_out[chunk] = (share[chunk] + share_in[chunk].astype(jnp.float32)).astype(jnp.bfloat16)
        place = lax.div(me, 2)

        @pl.when(even)
        def _():
            send(far_out.at[chunk], far_in.at[chunk, place], 4, part_recv.at[chunk, 1], (before, last))

        @pl.when(~even)
        def _():
            send(far_out.at[chunk], far_in.at[chunk, place], 4, part_recv.at[chunk, 0], (after, 0))

    for chunk in range(CHUNKS):
        part = piece(chunk)
        returned = jnp.concatenate(arrived(chunk, back_in, back_recv), axis=1)
        rims = mm_t(returned, ip[0 : 2 * rim, :]).astype(jnp.bfloat16)
        part_out[chunk, 0] = rims[:, rim:]
        part_out[chunk, 1] = rims[:, :rim]

        @pl.when(me < last)
        def _():
            send(part_out.at[chunk, 0], part_in.at[chunk, 0], 5, part_recv.at[chunk, 0], (tile, up))

        @pl.when(me > 0)
        def _():
            send(part_out.at[chunk, 1], part_in.at[chunk, 1], 5, part_recv.at[chunk, 1], (tile, down))

        result[part, :] = mm_t(returned, ip[2 * rim :, :])

    for chunk in range(CHUNKS):
        part = piece(chunk)
        for side, where, pick, end in ((0, lead, left_pick, 0), (1, tail, right_pick, last)):

            @pl.when(me != end)
            def _():
                drain(part_in.at[chunk, side], part_recv.at[chunk, side])
                result[part, where] += mm_t(part_in[chunk, side], pick)

            @pl.when(me == end)
            def _():
                drain(far_in.at[chunk], part_recv.at[chunk, side])
                total = result[part, where]
                for g in range(groups // 2):
                    total = total + mm_t(far_in[chunk, g], pick)
                result[part, where] = total

    drain(cell_out.at[:, :, 0:last], send_sem.at[0])
    drain(far_out, send_sem.at[4])
    drain(share_out, send_sem.at[7])
    pl.when(even)(lambda: drain(late_in, send_sem.at[1]))
    pl.when(~even)(lambda: drain(late_in.at[:, 0], send_sem.at[8]))

    pl.when(me == 0)(lambda: drain(far_in.at[:, 0 : groups // 2 - 1], send_sem.at[6]))
    pl.when(me == last)(lambda: drain(far_in, send_sem.at[1]))

    @pl.when((me == 0) | (me == last))
    def _():
        drain(edge_out.at[:, 0], send_sem.at[2])
        drain(rim_out.at[0:last], send_sem.at[3])
        drain(part_out.at[:, 0], send_sem.at[5])

    @pl.when((me != 0) & (me != last))
    def _():
        drain(edge_out, send_sem.at[2])
        drain(part_out, send_sem.at[5])


def in_hbm(array):
    return pltpu.with_memory_space_constraint(array, pltpu.HBM)


def on_device(tiles, groups, field, interp, conv_blocks, band_shift, owner, edge_index):
    rows, columns = field.shape
    extended, points = interp.shape
    rim = edge_index.shape[1]
    slots = conv_blocks.shape[0] * conv_blocks.shape[2]
    capacity = slots // groups
    height = rows // CHUNKS
    half, single = jnp.bfloat16, jnp.float32
    sides = pltpu.VMEM((CHUNKS, 2, height, rim), half)
    strip = pltpu.VMEM((CHUNKS, height, rim), half)
    cells = pltpu.VMEM((CHUNKS, groups, height, capacity), half)
    dma = pltpu.SemaphoreType.DMA
    anywhere = pl.BlockSpec(memory_space=pltpu.HBM)
    return pl.pallas_call(
        functools.partial(kernel, tiles, groups, rim),
        out_shape=jax.ShapeDtypeStruct(field.shape, single),
        in_specs=[anywhere] * 6,
        out_specs=pl.BlockSpec(memory_space=pltpu.VMEM),
        scratch_shapes=[
            pltpu.VMEM(field.shape, single),
            pltpu.VMEM(interp.shape, half),
            pltpu.VMEM(conv_blocks.shape, half),
            pltpu.VMEM((1, points), jnp.int32),
            pltpu.VMEM(edge_index.shape, jnp.int32),
            pltpu.VMEM(band_shift.shape, jnp.int32),
            pltpu.VMEM((extended, slots), half),
            pltpu.VMEM((slots, slots), half),
            pltpu.VMEM((slots, slots), half),
            pltpu.VMEM((rows, slots), single),
            sides, sides, strip, sides,
            pltpu.VMEM((groups, rim, capacity), half),
            pltpu.VMEM((2, rim, capacity), half),
            pltpu.VMEM((2, CHUNKS, groups, height, capacity), half),
            cells, cells,
            pltpu.VMEM((CHUNKS, height, rim), single),
            strip, strip, strip,
            pltpu.VMEM((CHUNKS, groups // 2, height, rim), half),
            sides, sides,
            pltpu.SemaphoreType.REGULAR((2,)), dma((8,)), dma((9,)), dma((CHUNKS, 2)), dma((1,)), dma((CHUNKS, 2)), dma((2,)), dma((CHUNKS,)), dma((CHUNKS,)), dma((CHUNKS,)),
            dma((CHUNKS, 2)),
        ],
        compiler_params=pltpu.CompilerParams(collective_id=0, has_side_effects=True, vmem_limit_bytes=53 * 2**20),
    )(field, interp, conv_blocks, *[in_hbm(small) for small in (owner.reshape(1, -1), edge_index, band_shift)])


def solution(mesh):
    return jax.shard_map(
        functools.partial(on_device, mesh.shape["tile"], mesh.shape["conv"]),
        mesh=mesh,
        in_specs=(
            P(None, ("tile", "conv")),
            P(("tile", "conv"), None),
            P(("tile", "conv"), None, None, None),
            P(("tile", "conv"), None),
            P(("tile", "conv"), None),
            P(("tile", "conv"), None),
        ),
        out_specs=P(None, ("tile", "conv")),
        check_vma=False,
    )
```

```python
import functools

import jax
import jax.numpy as jnp
from jax import lax
from jax.experimental import pallas as pl
from jax.experimental.pallas import tpu as pltpu
from jax.sharding import PartitionSpec as P

MESH = pl.DeviceIdType.MESH
CHUNKS = 2


def mm(left, right):
    return lax.dot_general(left, right, (((1,), (0,)), ((), ())), preferred_element_type=jnp.float32)


def mm_t(left, right):
    return lax.dot_general(left, right, (((1,), (1,)), ((), ())), preferred_element_type=jnp.float32)


def kernel(
    tiles, groups, rim, field_hbm, interp_hbm, blocks_hbm, owner_hbm, index_hbm, shift_hbm, result,
    field, interp, blocks, owner, index, shift, ip, conv, gram, base,
    edge_out, edge_in, relay, late_in, rim_out, rim_in, cell_out, slot_in, back_in, far_gram, share, share_in, far_out, far_in, part_out, part_in,
    ready, load_sem, send_sem, edge_recv, relay_recv, late_recv, rim_recv, slot_recv, back_recv, share_recv, part_recv,
):
    rows, columns = field.shape
    extended, points = interp.shape
    owned, bands, size = blocks.shape[0], blocks.shape[1], blocks.shape[2]
    slots = owned * size
    capacity = slots // groups
    height = rows // CHUNKS
    last = groups - 1
    tile, me = lax.axis_index("tile"), lax.axis_index("conv")
    after, before = lax.rem(tile + 1, tiles), lax.rem(tile + tiles - 1, tiles)
    up, down = lax.rem(me + 1, groups), lax.rem(me + last, groups)
    middle = groups // 2
    low = me < middle
    peers = [jnp.where(low, middle + k, middle - 1 - k) for k in range(middle)]
    peers += [lax.rem(me + k, middle) + jnp.where(low, 0, middle) for k in range(1, middle)]

    barrier = pltpu.get_barrier_semaphore()
    first_tile, last_tile = tile == 0, tile == tiles - 1
    odd = lax.rem(me, 2)
    even = odd == 0
    mate = me + 1 - 2 * odd

    def meet(lower, upper):
        return (upper == 0) | (lower == last) | (upper == lower - lax.rem(lower, 2))

    with_before = [meet(g, me) for g in range(groups)]
    with_after = [meet(me, g) for g in range(groups)]
    from_before = sum(jnp.where(met, 1, 0) for met in with_before)
    from_after = sum(jnp.where(met, 1, 0) for met in with_after)

    def signal(semaphore, target):
        pl.semaphore_signal(semaphore, inc=1, device_id=target, device_id_type=MESH)

    def tell(semaphore, there, met):
        for g in range(groups):
            pl.when(met[g])(functools.partial(signal, semaphore, (there, g)))

    def tell_before(semaphore):
        tell(semaphore, before, with_before)

    def tell_after(semaphore):
        tell(semaphore, after, with_after)

    pl.when(first_tile)(lambda: tell_before(barrier))
    pl.when(~last_tile)(lambda: tell_after(barrier))
    for peer in peers:
        signal(barrier, (tile, peer))

    def load(source, target, at):
        copy = pltpu.make_async_copy(source, target, load_sem.at[at])
        copy.start()
        return copy

    def drain(ref, semaphore):
        pltpu.make_async_copy(ref, ref, semaphore).wait()

    inner = slice(rim, columns - rim)
    lead, tail = slice(0, rim), slice(columns - rim, columns)
    load_index = load(index_hbm, index, 0)
    load_lead = load(field_hbm.at[:, lead], field.at[:, lead], 1)
    load_tail = load(field_hbm.at[:, tail], field.at[:, tail], 2)
    load_owner = load(owner_hbm, owner, 3)
    load_interp = load(interp_hbm, interp, 4)
    load_inner = load(field_hbm.at[:, inner], field.at[:, inner], 5)
    load_shift = load(shift_hbm, shift, 6)
    load_blocks = load(blocks_hbm, blocks, 7)

    def piece(chunk):
        return slice(chunk * height, (chunk + 1) * height)

    def send(source, target, arrival, place):
        pltpu.make_async_remote_copy(
            src_ref=source, dst_ref=target, send_sem=send_sem.at[0], recv_sem=arrival,
            device_id=place, device_id_type=MESH,
        ).start()

    def exchange(kind, chunk, in_ref, recv):
        for peer in peers:
            send(cell_out.at[kind, chunk, peer], in_ref.at[chunk, me], recv.at[chunk], (tile, peer))
        in_ref[chunk, me] = cell_out[kind, chunk, me]

    def arrived(chunk, in_ref, recv):
        drain(in_ref.at[chunk, 0:last], recv.at[chunk])
        return [in_ref[chunk, g] for g in range(groups)]

    pl.semaphore_wait(
        barrier, last + jnp.where(first_tile, 0, from_before) + jnp.where(last_tile, from_after, 0)
    )
    pl.when(~first_tile)(lambda: tell_before(ready.at[1]))
    pl.when(last_tile)(lambda: tell_after(ready.at[0]))

    load_index.wait()
    left_list, right_list = index[0:1, :], index[1:2, :]
    lines = lax.broadcasted_iota(jnp.int32, (rim, rim), 0)
    left_pick = (lines == left_list).astype(jnp.float32).astype(jnp.bfloat16)
    right_pick = (lines + (columns - rim) == right_list).astype(jnp.float32).astype(jnp.bfloat16)
    load_lead.wait()
    load_tail.wait()
    for chunk in range(CHUNKS):
        part = piece(chunk)
        edge_out[chunk, 0] = mm(field[part, tail].astype(jnp.bfloat16), right_pick).astype(jnp.bfloat16)
        edge_out[chunk, 1] = mm(field[part, lead].astype(jnp.bfloat16), left_pick).astype(jnp.bfloat16)

    for chunk in range(CHUNKS):

        @pl.when(me < last)
        def _():
            send(edge_out.at[chunk, 0], edge_in.at[chunk, 0], edge_recv.at[chunk, 0], (tile, up))

        @pl.when(me > 0)
        def _():
            send(edge_out.at[chunk, 1], edge_in.at[chunk, 1], edge_recv.at[chunk, 1], (tile, down))

    @pl.when((me == 0) & ~last_tile)
    def _():
        relay[...] = edge_out[:, 1]
        for g in range(2, groups, 2):
            send(edge_out.at[:, 1], relay, relay_recv.at[0], (tile, g))

    def late_right():
        for chunk in range(CHUNKS):
            for g in range(1, groups, 2):
                send(edge_out.at[chunk, 0], late_in.at[chunk, 0], late_recv.at[chunk, 0], (after, g))

    pl.when((me == last) & last_tile)(late_right)

    load_owner.wait()
    owners = owner[...]
    choose = (owners == lax.broadcasted_iota(jnp.int32, (-(-groups // 8) * 8, points), 0)).astype(jnp.float32)
    order = lax.broadcasted_iota(jnp.int32, (points, points), 0) < lax.broadcasted_iota(
        jnp.int32, (points, points), 1
    )
    ranks = mm(choose.astype(jnp.bfloat16), order.astype(jnp.float32).astype(jnp.bfloat16))
    rank = jnp.sum(ranks * choose, axis=0, keepdims=True)
    slot = owners * capacity + rank.astype(jnp.int32)
    placement = (slot == lax.broadcasted_iota(jnp.int32, (slots, points), 0)).astype(jnp.float32)
    placement = placement.astype(jnp.bfloat16)
    load_interp.wait()
    ip[0:rim, :] = mm_t(interp[0:rim, :], placement).astype(jnp.bfloat16)
    ip[rim : 2 * rim, :] = mm_t(interp[extended - rim :, :], placement).astype(jnp.bfloat16)

    def spread(side, at):
        for g in range(groups):
            rim_out[g] = ip[side * rim : (side + 1) * rim, g * capacity : (g + 1) * capacity]
        rim_in[side] = rim_out[at]
        for chunk in range(CHUNKS):
            edge_in[chunk, side] = jnp.zeros((height, rim), jnp.bfloat16)

    pl.when(me == 0)(functools.partial(spread, 0, 0))
    pl.when(me == last)(functools.partial(spread, 1, last))

    @pl.when(me == 0)
    def _():
        for g in range(1, groups):
            send(rim_out.at[g], rim_in.at[0], rim_recv.at[0], (tile, g))

    @pl.when(me == last)
    def _():
        for g in range(last):
            send(rim_out.at[g], rim_in.at[1], rim_recv.at[1], (tile, g))

    ip[2 * rim :, :] = mm_t(interp[rim : extended - rim, :], placement).astype(jnp.bfloat16)
    load_inner.wait()
    base[...] = mm(field[...].astype(jnp.bfloat16), ip[2 * rim :, :])

    for chunk in range(CHUNKS):
        pl.when(me > 0)(lambda: drain(edge_in.at[chunk, 0], edge_recv.at[chunk, 0]))
        pl.when(me < last)(lambda: drain(edge_in.at[chunk, 1], edge_recv.at[chunk, 1]))
        edges = jnp.concatenate([edge_in[chunk, 0], edge_in[chunk, 1]], axis=1)
        subgrid = (base[piece(chunk), :] + mm(edges, ip[0 : 2 * rim, :])).astype(jnp.bfloat16)
        for g in range(groups):
            cell_out[0, chunk, g] = subgrid[:, g * capacity : (g + 1) * capacity]
        exchange(0, chunk, slot_in, slot_recv)

    @pl.when((me == last) & ~last_tile)
    def _():
        pl.semaphore_wait(ready.at[1], from_after)
        late_right()

    def late_left(source, cores):
        for chunk in range(CHUNKS):
            for g in cores:
                send(source.at[chunk], late_in.at[chunk, 1], late_recv.at[chunk, 1], (before, g))

    pl.when(last_tile & (me == 0))(lambda: late_left(edge_out.at[:, 1], range(groups)))
    pl.when(even & (me != 0) & ~last_tile)(lambda: drain(relay, relay_recv.at[0]))

    @pl.when(even & ~last_tile)
    def _():
        pl.when(first_tile)(lambda: pl.semaphore_wait(ready.at[0], from_before))
        late_left(relay, (me, me + 1))

    load_shift.wait()
    load_blocks.wait()
    for j in range(owned):
        for s in range(owned):
            total = jnp.zeros((size, size), jnp.float32)
            for c in range(bands):
                reads = lax.rem(j + shift[j : j + 1, c : c + 1], owned) == s
                total = total + jnp.where(reads, 1.0, 0.0) * blocks[j, c].astype(jnp.float32)
            conv[s * size : (s + 1) * size, j * size : (j + 1) * size] = total.astype(jnp.bfloat16)
    gram[...] = mm_t(conv[...], conv[...]).astype(jnp.bfloat16)

    pl.when(me > 0)(lambda: drain(rim_in.at[0], rim_recv.at[0]))
    pl.when(me < last)(lambda: drain(rim_in.at[1], rim_recv.at[1]))
    for side, g in ((0, 0), (1, last)):
        product = mm_t(gram[:, g * capacity : (g + 1) * capacity], rim_in[side])
        far_gram[:, side * rim : (side + 1) * rim] = product.astype(jnp.bfloat16)

    pl.when(~even & first_tile)(lambda: pl.semaphore_wait(ready.at[0], from_before))
    pl.when((me != last) & ~last_tile)(lambda: pl.semaphore_wait(ready.at[1], from_after))

    @pl.when(~even)
    def _():
        for chunk in range(CHUNKS):
            drain(late_in.at[chunk, 0], late_recv.at[chunk, 0])
            send(late_in.at[chunk, 0], late_in.at[chunk, 0], late_recv.at[chunk, 0], (tile, mate))

    for chunk in range(CHUNKS):
        cells = arrived(chunk, slot_in, slot_recv)
        pl.when(even)(lambda: drain(late_in.at[chunk, 0], late_recv.at[chunk, 0]))
        drain(late_in.at[chunk, 1], late_recv.at[chunk, 1])
        for side, g in ((0, 0), (1, last)):
            cells[g] = (cells[g].astype(jnp.float32) + mm(late_in[chunk, side], rim_in[side])).astype(jnp.bfloat16)
        gathered = jnp.concatenate(cells, axis=1)
        far = mm(gathered, far_gram[...])
        far_out[chunk, 1] = far[:, rim:].astype(jnp.bfloat16)
        send(far_out.at[chunk, 1], far_in.at[chunk, me], part_recv.at[chunk, 0], (after, 0))
        share[chunk] = far[:, :rim]

        @pl.when(~even)
        def _():
            far_out[chunk, 0] = share[chunk].astype(jnp.bfloat16)
            send(far_out.at[chunk, 0], share_in.at[chunk], share_recv.at[chunk], (tile, mate))

        adjoint = mm(gathered, gram[...]).astype(jnp.bfloat16)
        for g in range(groups):
            cell_out[1, chunk, g] = adjoint[:, g * capacity : (g + 1) * capacity]
        exchange(1, chunk, back_in, back_recv)

    @pl.when(even)
    def _():
        for chunk in range(CHUNKS):
            drain(share_in.at[chunk], share_recv.at[chunk])
            far_out[chunk, 0] = (share[chunk] + share_in[chunk].astype(jnp.float32)).astype(jnp.bfloat16)
            send(far_out.at[chunk, 0], far_in.at[chunk, lax.div(me, 2)], part_recv.at[chunk, 1], (before, last))

    for chunk in range(CHUNKS):
        part = piece(chunk)
        returned = jnp.concatenate(arrived(chunk, back_in, back_recv), axis=1)
        rims = mm_t(returned, ip[0 : 2 * rim, :]).astype(jnp.bfloat16)
        part_out[chunk, 0] = rims[:, rim:]
        part_out[chunk, 1] = rims[:, :rim]

        @pl.when(me < last)
        def _():
            send(part_out.at[chunk, 0], part_in.at[chunk, 0], part_recv.at[chunk, 0], (tile, up))

        @pl.when(me > 0)
        def _():
            send(part_out.at[chunk, 1], part_in.at[chunk, 1], part_recv.at[chunk, 1], (tile, down))

        result[part, :] = mm_t(returned, ip[2 * rim :, :])

    borders = [
        (chunk, piece(chunk), *border)
        for chunk in range(CHUNKS)
        for border in ((0, lead, left_pick, 0), (1, tail, right_pick, last))
    ]
    for chunk, part, side, where, pick, end in borders:

        @pl.when(me != end)
        def _():
            drain(part_in.at[chunk, side], part_recv.at[chunk, side])
            result[part, where] += mm_t(part_in[chunk, side], pick)

    for chunk, part, side, where, pick, end in borders:
        shares = middle if side else groups

        @pl.when(me == end)
        def _():
            drain(far_in.at[chunk, 0:shares], part_recv.at[chunk, side])
            total = result[part, where]
            for g in range(shares):
                total = total + mm_t(far_in[chunk, g], pick)
            result[part, where] = total

    drain(cell_out.at[:, :, 0:last], send_sem.at[0])
    drain(far_out, send_sem.at[0])
    pl.when(even & ~last_tile)(lambda: drain(late_in, send_sem.at[0]))
    pl.when((me == 0) & last_tile)(lambda: drain(far_in, send_sem.at[0]))
    pl.when(~even)(lambda: drain(late_in.at[:, 0], send_sem.at[0]))

    pl.when((me == 0) & ~last_tile)(lambda: drain(far_in.at[:, 0 : groups // 2 - 1], send_sem.at[0]))
    pl.when(me == last)(lambda: drain(far_in.at[:, 0 : groups // 2], send_sem.at[0]))

    @pl.when((me == 0) | (me == last))
    def _():
        drain(edge_out.at[:, 0], send_sem.at[0])
        drain(rim_out.at[0:last], send_sem.at[0])
        drain(part_out.at[:, 0], send_sem.at[0])

    @pl.when((me != 0) & (me != last))
    def _():
        drain(edge_out, send_sem.at[0])
        drain(part_out, send_sem.at[0])


def in_hbm(array):
    return pltpu.with_memory_space_constraint(array, pltpu.HBM)


def on_device(tiles, groups, field, interp, conv_blocks, band_shift, owner, edge_index):
    rows, columns = field.shape
    extended, points = interp.shape
    rim = edge_index.shape[1]
    slots = conv_blocks.shape[0] * conv_blocks.shape[2]
    capacity = slots // groups
    height = rows // CHUNKS
    half, single = jnp.bfloat16, jnp.float32
    sides = pltpu.VMEM((CHUNKS, 2, height, rim), half)
    strip = pltpu.VMEM((CHUNKS, height, rim), half)
    cells = pltpu.VMEM((CHUNKS, groups, height, capacity), half)
    dma = pltpu.SemaphoreType.DMA
    anywhere = pl.BlockSpec(memory_space=pltpu.HBM)
    return pl.pallas_call(
        functools.partial(kernel, tiles, groups, rim),
        out_shape=jax.ShapeDtypeStruct(field.shape, single),
        in_specs=[anywhere] * 6,
        out_specs=pl.BlockSpec(memory_space=pltpu.VMEM),
        scratch_shapes=[
            pltpu.VMEM(field.shape, single),
            pltpu.VMEM(interp.shape, half),
            pltpu.VMEM(conv_blocks.shape, half),
            pltpu.VMEM((1, points), jnp.int32),
            pltpu.VMEM(edge_index.shape, jnp.int32),
            pltpu.VMEM(band_shift.shape, jnp.int32),
            pltpu.VMEM((extended, slots), half),
            pltpu.VMEM((slots, slots), half),
            pltpu.VMEM((slots, slots), half),
            pltpu.VMEM((rows, slots), single),
            sides, sides, strip, sides,
            pltpu.VMEM((groups, rim, capacity), half),
            pltpu.VMEM((2, rim, capacity), half),
            pltpu.VMEM((2, CHUNKS, groups, height, capacity), half),
            cells, cells,
            pltpu.VMEM((slots, 2 * rim), half),
            pltpu.VMEM((CHUNKS, height, rim), single),
            strip,
            sides,
            pltpu.VMEM((CHUNKS, groups, height, rim), half),
            sides, sides,
            pltpu.SemaphoreType.REGULAR((2,)), dma((8,)), dma((1,)), dma((CHUNKS, 2)), dma((1,)), dma((CHUNKS, 2)), dma((2,)), dma((CHUNKS,)), dma((CHUNKS,)), dma((CHUNKS,)),
            dma((CHUNKS, 2)),
        ],
        compiler_params=pltpu.CompilerParams(collective_id=0, has_side_effects=True, vmem_limit_bytes=53 * 2**20),
    )(field, interp, conv_blocks, *[in_hbm(small) for small in (owner.reshape(1, -1), edge_index, band_shift)])


def solution(mesh):
    return jax.shard_map(
        functools.partial(on_device, mesh.shape["tile"], mesh.shape["conv"]),
        mesh=mesh,
        in_specs=(
            P(None, ("tile", "conv")),
            P(("tile", "conv"), None),
            P(("tile", "conv"), None, None, None),
            P(("tile", "conv"), None),
            P(("tile", "conv"), None),
            P(("tile", "conv"), None),
        ),
        out_specs=P(None, ("tile", "conv")),
        check_vma=False,
    )
```

```python
import functools

import jax
import jax.numpy as jnp
from jax import lax
from jax.experimental import pallas as pl
from jax.experimental.pallas import tpu as pltpu
from jax.sharding import PartitionSpec as P

MESH = pl.DeviceIdType.MESH
CHUNKS = 2
FAR = 2


def mm(left, right):
    return lax.dot_general(left, right, (((1,), (0,)), ((), ())), preferred_element_type=jnp.float32)


def mm_t(left, right):
    return lax.dot_general(left, right, (((1,), (1,)), ((), ())), preferred_element_type=jnp.float32)


def kernel(
    tiles, groups, rim, field_hbm, interp_hbm, blocks_hbm, owner_hbm, index_hbm, shift_hbm, result,
    field, interp, blocks, owner, index, shift, ip, conv, gram, base, returned,
    edge_out, edge_in, relay, late_in, rim_out, rim_in, cell_out, slot_in, back_in, gathered, far_gram, share, share_in, far_out, far_in, part_out, part_in,
    ready, load_sem, send_sem, edge_recv, relay_recv, late_recv, rim_recv, slot_recv, back_recv, share_recv, part_recv, far_recv,
):
    rows, columns = field.shape
    extended, points = interp.shape
    owned, bands, size = blocks.shape[0], blocks.shape[1], blocks.shape[2]
    slots = owned * size
    capacity = slots // groups
    height = rows // CHUNKS
    step = CHUNKS // FAR
    last = groups - 1
    tile, me = lax.axis_index("tile"), lax.axis_index("conv")
    after, before = lax.rem(tile + 1, tiles), lax.rem(tile + tiles - 1, tiles)
    up, down = lax.rem(me + 1, groups), lax.rem(me + last, groups)
    middle = groups // 2
    low = me < middle
    peers = [jnp.where(low, middle + k, middle - 1 - k) for k in range(middle)]
    peers += [lax.rem(me + k, middle) + jnp.where(low, 0, middle) for k in range(1, middle)]

    barrier = pltpu.get_barrier_semaphore()
    first_tile, last_tile = tile == 0, tile == tiles - 1
    odd = lax.rem(me, 2)
    even = odd == 0
    mate = me + 1 - 2 * odd

    def meet(lower, upper):
        return (upper == 0) | (lower == last) | (upper == lower - lax.rem(lower, 2))

    with_before = [meet(g, me) for g in range(groups)]
    with_after = [meet(me, g) for g in range(groups)]
    from_before = sum(jnp.where(met, 1, 0) for met in with_before)
    from_after = sum(jnp.where(met, 1, 0) for met in with_after)

    def signal(semaphore, target):
        pl.semaphore_signal(semaphore, inc=1, device_id=target, device_id_type=MESH)

    def tell(semaphore, there, met):
        for g in range(groups):
            pl.when(met[g])(functools.partial(signal, semaphore, (there, g)))

    def tell_before(semaphore):
        tell(semaphore, before, with_before)

    def tell_after(semaphore):
        tell(semaphore, after, with_after)

    pl.when(first_tile)(lambda: tell_before(barrier))
    pl.when(~last_tile)(lambda: tell_after(barrier))
    for peer in peers:
        signal(barrier, (tile, peer))

    def load(source, target, at):
        copy = pltpu.make_async_copy(source, target, load_sem.at[at])
        copy.start()
        return copy

    def drain(ref, semaphore):
        pltpu.make_async_copy(ref, ref, semaphore).wait()

    inner = slice(rim, columns - rim)
    lead, tail = slice(0, rim), slice(columns - rim, columns)
    load_index = load(index_hbm, index, 0)
    load_lead = load(field_hbm.at[:, lead], field.at[:, lead], 1)
    load_tail = load(field_hbm.at[:, tail], field.at[:, tail], 2)
    load_owner = load(owner_hbm, owner, 3)
    load_interp = load(interp_hbm, interp, 4)
    load_inner = load(field_hbm.at[:, inner], field.at[:, inner], 5)
    load_shift = load(shift_hbm, shift, 6)
    load_blocks = load(blocks_hbm, blocks, 7)

    def piece(chunk):
        return slice(chunk * height, (chunk + 1) * height)

    def send(source, target, arrival, place):
        pltpu.make_async_remote_copy(
            src_ref=source, dst_ref=target, send_sem=send_sem.at[0], recv_sem=arrival,
            device_id=place, device_id_type=MESH,
        ).start()

    def exchange(kind, chunk, in_ref, recv):
        for peer in peers:
            send(cell_out.at[kind, chunk, peer], in_ref.at[chunk, me], recv.at[chunk], (tile, peer))
        in_ref[chunk, me] = cell_out[kind, chunk, me]

    def arrived(chunk, in_ref, recv):
        drain(in_ref.at[chunk, 0:last], recv.at[chunk])
        return [in_ref[chunk, g] for g in range(groups)]

    pl.semaphore_wait(
        barrier, last + jnp.where(first_tile, 0, from_before) + jnp.where(last_tile, from_after, 0)
    )
    pl.when(~first_tile)(lambda: tell_before(ready.at[1]))
    pl.when(last_tile)(lambda: tell_after(ready.at[0]))

    load_index.wait()
    left_list, right_list = index[0:1, :], index[1:2, :]
    lines = lax.broadcasted_iota(jnp.int32, (rim, rim), 0)
    left_pick = (lines == left_list).astype(jnp.float32).astype(jnp.bfloat16)
    right_pick = (lines + (columns - rim) == right_list).astype(jnp.float32).astype(jnp.bfloat16)
    load_lead.wait()
    load_tail.wait()
    for chunk in range(CHUNKS):
        part = piece(chunk)
        edge_out[chunk, 0] = mm(field[part, tail].astype(jnp.bfloat16), right_pick).astype(jnp.bfloat16)
        edge_out[chunk, 1] = mm(field[part, lead].astype(jnp.bfloat16), left_pick).astype(jnp.bfloat16)

    for chunk in range(CHUNKS):

        @pl.when(me < last)
        def _():
            send(edge_out.at[chunk, 0], edge_in.at[chunk, 0], edge_recv.at[chunk], (tile, up))

        @pl.when(me > 0)
        def _():
            send(edge_out.at[chunk, 1], edge_in.at[chunk, 1], edge_recv.at[chunk], (tile, down))

    @pl.when((me == 0) & ~last_tile)
    def _():
        relay[...] = edge_out[:, 1]
        for g in range(2, groups, 2):
            send(edge_out.at[:, 1], relay, relay_recv.at[0], (tile, g))

    def late_right():
        for part in range(FAR):
            for g in range(1, groups, 2):
                source = edge_out.at[part * step : (part + 1) * step, 0]
                send(source, late_in.at[part, 0], late_recv.at[part, 0], (after, g))

    pl.when((me == last) & last_tile)(late_right)

    load_owner.wait()
    owners = owner[...]
    choose = (owners == lax.broadcasted_iota(jnp.int32, (-(-groups // 8) * 8, points), 0)).astype(jnp.float32)
    order = lax.broadcasted_iota(jnp.int32, (points, points), 0) < lax.broadcasted_iota(
        jnp.int32, (points, points), 1
    )
    ranks = mm(choose.astype(jnp.bfloat16), order.astype(jnp.float32).astype(jnp.bfloat16))
    rank = jnp.sum(ranks * choose, axis=0, keepdims=True)
    slot = owners * capacity + rank.astype(jnp.int32)
    placement = (slot == lax.broadcasted_iota(jnp.int32, (slots, points), 0)).astype(jnp.float32)
    placement = placement.astype(jnp.bfloat16)
    load_interp.wait()
    ip[0:rim, :] = mm_t(interp[0:rim, :], placement).astype(jnp.bfloat16)
    ip[rim : 2 * rim, :] = mm_t(interp[extended - rim :, :], placement).astype(jnp.bfloat16)

    def spread(side, at):
        for g in range(groups):
            rim_out[g] = ip[side * rim : (side + 1) * rim, g * capacity : (g + 1) * capacity]
        rim_in[side] = rim_out[at]
        for chunk in range(CHUNKS):
            edge_in[chunk, side] = jnp.zeros((height, rim), jnp.bfloat16)

    pl.when(me == 0)(functools.partial(spread, 0, 0))
    pl.when(me == last)(functools.partial(spread, 1, last))

    @pl.when(me == 0)
    def _():
        for g in range(1, groups):
            send(rim_out.at[g], rim_in.at[0], rim_recv.at[0], (tile, g))

    @pl.when(me == last)
    def _():
        for g in range(last):
            send(rim_out.at[g], rim_in.at[1], rim_recv.at[0], (tile, g))

    ip[2 * rim :, :] = mm_t(interp[rim : extended - rim, :], placement).astype(jnp.bfloat16)
    load_inner.wait()
    base[...] = mm(field[...].astype(jnp.bfloat16), ip[2 * rim :, :])

    load_shift.wait()
    load_blocks.wait()

    def build_gram():
        for j in range(owned):
            for s in range(owned):
                total = jnp.zeros((size, size), jnp.float32)
                for c in range(bands):
                    reads = lax.rem(j + shift[j : j + 1, c : c + 1], owned) == s
                    total = total + jnp.where(reads, 1.0, 0.0) * blocks[j, c].astype(jnp.float32)
                conv[s * size : (s + 1) * size, j * size : (j + 1) * size] = total.astype(jnp.bfloat16)
        gram[...] = mm_t(conv[...], conv[...]).astype(jnp.bfloat16)

    outer = (me == 0) | (me == last)
    pl.when(~outer)(build_gram)

    for chunk in range(CHUNKS):
        pl.when(outer)(lambda: drain(edge_in.at[chunk, 0], edge_recv.at[chunk]))
        pl.when(~outer)(lambda: drain(edge_in.at[chunk], edge_recv.at[chunk]))
        edges = jnp.concatenate([edge_in[chunk, 0], edge_in[chunk, 1]], axis=1)
        subgrid = (base[piece(chunk), :] + mm(edges, ip[0 : 2 * rim, :])).astype(jnp.bfloat16)
        for g in range(groups):
            cell_out[0, chunk, g] = subgrid[:, g * capacity : (g + 1) * capacity]
        exchange(0, chunk, slot_in, slot_recv)

    @pl.when((me == last) & ~last_tile)
    def _():
        pl.semaphore_wait(ready.at[1], from_after)
        late_right()

    def late_left(source, cores):
        for part in range(FAR):
            for g in cores:
                rows_of = source.at[part * step : (part + 1) * step]
                send(rows_of, late_in.at[part, 1], late_recv.at[part, 1], (before, g))

    pl.when(last_tile & (me == 0))(lambda: late_left(edge_out.at[:, 1], range(groups)))
    pl.when(even & (me != 0) & ~last_tile)(lambda: drain(relay, relay_recv.at[0]))

    @pl.when(even & ~last_tile)
    def _():
        pl.when(first_tile)(lambda: pl.semaphore_wait(ready.at[0], from_before))
        late_left(relay, (me, me + 1))

    pl.when(outer)(build_gram)

    pl.when(outer)(lambda: drain(rim_in.at[0], rim_recv.at[0]))
    pl.when(~outer)(lambda: drain(rim_in, rim_recv.at[0]))
    for side, g in ((0, 0), (1, last)):
        product = mm_t(gram[:, g * capacity : (g + 1) * capacity], rim_in[side])
        far_gram[:, side * rim : (side + 1) * rim] = product.astype(jnp.bfloat16)

    pl.when(~even & first_tile)(lambda: pl.semaphore_wait(ready.at[0], from_before))
    pl.when((me != last) & ~last_tile)(lambda: pl.semaphore_wait(ready.at[1], from_after))

    def pass_on(part):
        drain(late_in.at[part, 0], late_recv.at[part, 0])
        send(late_in.at[part, 0], late_in.at[part, 0], late_recv.at[part, 0], (tile, mate))

    @pl.when(~even)
    def _():
        for part in range(FAR):
            pass_on(part)

    for chunk in range(CHUNKS):
        far_part, row = chunk // step, chunk % step
        if row == 0:
            pl.when(even)(lambda: drain(late_in.at[far_part, 0], late_recv.at[far_part, 0]))
            drain(late_in.at[far_part, 1], late_recv.at[far_part, 1])
        added = [mm(late_in[far_part, side, row], rim_in[side]) for side in range(2)]
        cells = arrived(chunk, slot_in, slot_recv)
        for side, g in ((0, 0), (1, last)):
            cells[g] = (cells[g].astype(jnp.float32) + added[side]).astype(jnp.bfloat16)
        gathered[chunk] = jnp.concatenate(cells, axis=1)

        def far_shares():
            far = mm(gathered[chunk], far_gram[...])
            far_out[chunk, 1] = far[:, rim:].astype(jnp.bfloat16)
            send(far_out.at[chunk, 1], far_in.at[chunk, me], far_recv.at[chunk], (after, 0))
            share[chunk] = far[:, :rim]

            @pl.when(~even)
            def _():
                far_out[chunk, 0] = share[chunk].astype(jnp.bfloat16)
                send(far_out.at[chunk, 0], share_in.at[chunk], share_recv.at[0], (tile, mate))

        pl.when(last_tile)(far_shares)
        adjoint = mm(gathered[chunk], gram[...]).astype(jnp.bfloat16)
        for g in range(groups):
            cell_out[1, chunk, g] = adjoint[:, g * capacity : (g + 1) * capacity]
        exchange(1, chunk, back_in, back_recv)
        pl.when(~last_tile)(far_shares)

    @pl.when(even)
    def _():
        drain(share_in, share_recv.at[0])
        far_out[:, 0] = (share[...] + share_in[...].astype(jnp.float32)).astype(jnp.bfloat16)
        send(far_out.at[:, 0], far_in.at[:, lax.div(me, 2)], far_recv.at[0], (before, last))

    for chunk in range(CHUNKS):
        back = jnp.concatenate(arrived(chunk, back_in, back_recv), axis=1)
        returned[chunk * height : (chunk + 1) * height, :] = back
        rims = mm_t(back, ip[0 : 2 * rim, :]).astype(jnp.bfloat16)
        part_out[chunk, 0] = rims[:, rim:]
        part_out[chunk, 1] = rims[:, :rim]

        @pl.when(me < last)
        def _():
            send(part_out.at[chunk, 0], part_in.at[chunk, 0], part_recv.at[chunk], (tile, up))

        @pl.when(me > 0)
        def _():
            send(part_out.at[chunk, 1], part_in.at[chunk, 1], part_recv.at[chunk], (tile, down))

        if chunk % step == step - 1:
            part = slice((chunk + 1 - step) * height, (chunk + 1) * height)
            result[part, :] = mm_t(returned[part, :], ip[2 * rim :, :])

    for chunk in range(CHUNKS):
        part = piece(chunk)
        pl.when(outer)(lambda: drain(part_in.at[chunk, 0], part_recv.at[chunk]))
        pl.when(~outer)(lambda: drain(part_in.at[chunk], part_recv.at[chunk]))

        @pl.when(me > 0)
        def _():
            result[part, lead] += mm_t(part_in[chunk, 0], left_pick)

        @pl.when(me < last)
        def _():
            result[part, tail] += mm_t(part_in[chunk, 1], right_pick)

    def add_shares(chunk, where, pick, shares):
        arrived_shares = jnp.concatenate([far_in[chunk, g] for g in range(shares)], axis=1)
        result[piece(chunk), where] += mm_t(arrived_shares, jnp.concatenate([pick] * shares, axis=1))

    @pl.when(me == 0)
    def _():
        for chunk in range(CHUNKS):
            drain(far_in.at[chunk], far_recv.at[chunk])
            add_shares(chunk, lead, left_pick, groups)

    @pl.when(me == last)
    def _():
        drain(far_in.at[:, 0:middle], far_recv.at[0])
        for chunk in range(CHUNKS):
            add_shares(chunk, tail, right_pick, middle)

    drain(cell_out.at[:, :, 0:last], send_sem.at[0])
    drain(far_out, send_sem.at[0])
    pl.when(even & ~last_tile)(lambda: drain(late_in, send_sem.at[0]))
    pl.when((me == 0) & last_tile)(lambda: drain(far_in, send_sem.at[0]))
    pl.when(~even)(lambda: drain(late_in.at[:, 0], send_sem.at[0]))

    pl.when((me == 0) & ~last_tile)(lambda: drain(far_in.at[:, 0 : groups // 2 - 1], send_sem.at[0]))
    pl.when(me == last)(lambda: drain(far_in.at[:, 0 : groups // 2], send_sem.at[0]))

    @pl.when((me == 0) | (me == last))
    def _():
        drain(edge_out.at[:, 0], send_sem.at[0])
        drain(rim_out.at[0:last], send_sem.at[0])
        drain(part_out.at[:, 0], send_sem.at[0])

    @pl.when((me != 0) & (me != last))
    def _():
        drain(edge_out, send_sem.at[0])
        drain(part_out, send_sem.at[0])


def in_hbm(array):
    return pltpu.with_memory_space_constraint(array, pltpu.HBM)


def on_device(tiles, groups, field, interp, conv_blocks, band_shift, owner, edge_index):
    rows, columns = field.shape
    extended, points = interp.shape
    rim = edge_index.shape[1]
    slots = conv_blocks.shape[0] * conv_blocks.shape[2]
    capacity = slots // groups
    height = rows // CHUNKS
    half, single = jnp.bfloat16, jnp.float32
    sides = pltpu.VMEM((CHUNKS, 2, height, rim), half)
    strip = pltpu.VMEM((CHUNKS, height, rim), half)
    cells = pltpu.VMEM((CHUNKS, groups, height, capacity), half)
    dma = pltpu.SemaphoreType.DMA
    anywhere = pl.BlockSpec(memory_space=pltpu.HBM)
    return pl.pallas_call(
        functools.partial(kernel, tiles, groups, rim),
        out_shape=jax.ShapeDtypeStruct(field.shape, single),
        in_specs=[anywhere] * 6,
        out_specs=pl.BlockSpec(memory_space=pltpu.VMEM),
        scratch_shapes=[
            pltpu.VMEM(field.shape, single),
            pltpu.VMEM(interp.shape, half),
            pltpu.VMEM(conv_blocks.shape, half),
            pltpu.VMEM((1, points), jnp.int32),
            pltpu.VMEM(edge_index.shape, jnp.int32),
            pltpu.VMEM(band_shift.shape, jnp.int32),
            pltpu.VMEM((extended, slots), half),
            pltpu.VMEM((slots, slots), half),
            pltpu.VMEM((slots, slots), half),
            pltpu.VMEM((rows, slots), single),
            pltpu.VMEM((rows, slots), half),
            sides, sides, strip, pltpu.VMEM((FAR, 2, CHUNKS // FAR, height, rim), half),
            pltpu.VMEM((groups, rim, capacity), half),
            pltpu.VMEM((2, rim, capacity), half),
            pltpu.VMEM((2, CHUNKS, groups, height, capacity), half),
            cells, cells,
            pltpu.VMEM((CHUNKS, height, slots), half),
            pltpu.VMEM((slots, 2 * rim), half),
            pltpu.VMEM((CHUNKS, height, rim), single),
            strip,
            sides,
            pltpu.VMEM((CHUNKS, groups, height, rim), half),
            sides, sides,
            pltpu.SemaphoreType.REGULAR((2,)), dma((8,)), dma((1,)), dma((CHUNKS,)), dma((1,)), dma((FAR, 2)),
            dma((1,)), dma((CHUNKS,)), dma((CHUNKS,)), dma((1,)), dma((CHUNKS,)), dma((CHUNKS,)),
        ],
        compiler_params=pltpu.CompilerParams(collective_id=0, has_side_effects=True, vmem_limit_bytes=53 * 2**20),
    )(field, interp, conv_blocks, *[in_hbm(small) for small in (owner.reshape(1, -1), edge_index, band_shift)])


def solution(mesh):
    return jax.shard_map(
        functools.partial(on_device, mesh.shape["tile"], mesh.shape["conv"]),
        mesh=mesh,
        in_specs=(
            P(None, ("tile", "conv")),
            P(("tile", "conv"), None),
            P(("tile", "conv"), None, None, None),
            P(("tile", "conv"), None),
            P(("tile", "conv"), None),
            P(("tile", "conv"), None),
        ),
        out_specs=P(None, ("tile", "conv")),
        check_vma=False,
    )
```

```python
import functools

import jax
import jax.numpy as jnp
from jax import lax
from jax.experimental import pallas as pl
from jax.experimental.pallas import tpu as pltpu
from jax.sharding import PartitionSpec as P

MESH = pl.DeviceIdType.MESH
CHUNKS = 2
FAR = 2


def mm(left, right):
    return lax.dot_general(left, right, (((1,), (0,)), ((), ())), preferred_element_type=jnp.float32)


def mm_t(left, right):
    return lax.dot_general(left, right, (((1,), (1,)), ((), ())), preferred_element_type=jnp.float32)


def kernel(
    tiles, groups, rim, field_hbm, interp_hbm, blocks_hbm, owner_hbm, index_hbm, shift_hbm, result,
    field, interp, blocks, owner, index, shift, ip, conv, gram, base, returned,
    edge_out, edge_in, relay, late_in, rim_out, rim_in, cell_out, slot_in, back_in, gathered, far_gram, share, share_in, far_out, far_in, part_out, part_in,
    ready, load_sem, send_sem, edge_recv, relay_recv, late_recv, rim_recv, slot_recv, back_recv, share_recv, part_recv, far_recv,
):
    rows, columns = field.shape
    extended, points = interp.shape
    owned, bands, size = blocks.shape[0], blocks.shape[1], blocks.shape[2]
    slots = owned * size
    capacity = slots // groups
    height = rows // CHUNKS
    step = CHUNKS // FAR
    last = groups - 1
    tile, me = lax.axis_index("tile"), lax.axis_index("conv")
    after, before = lax.rem(tile + 1, tiles), lax.rem(tile + tiles - 1, tiles)
    up, down = lax.rem(me + 1, groups), lax.rem(me + last, groups)
    middle = groups // 2
    low = me < middle
    peers = [jnp.where(low, middle + k, middle - 1 - k) for k in range(middle)]
    peers += [lax.rem(me + k, middle) + jnp.where(low, 0, middle) for k in range(1, middle)]

    barrier = pltpu.get_barrier_semaphore()
    first_tile, last_tile = tile == 0, tile == tiles - 1
    odd = lax.rem(me, 2)
    even = odd == 0
    mate = me + 1 - 2 * odd
    pre_last = (tile == tiles - 2) & ~first_tile
    hands_right = pre_last & ~even & (me != last)
    hands_on = (first_tile & ~even) | (~first_tile & ~last_tile & even)

    def meet(lower, upper):
        return (upper == 0) | (lower == last) | (lax.div(lower, 2) == lax.div(upper, 2))

    with_before = [meet(g, me) for g in range(groups)]
    with_after = [meet(me, g) for g in range(groups)]
    from_before = sum(jnp.where(met, 1, 0) for met in with_before)
    from_after = sum(jnp.where(met, 1, 0) for met in with_after)

    def signal(semaphore, target):
        pl.semaphore_signal(semaphore, inc=1, device_id=target, device_id_type=MESH)

    def tell(semaphore, there, met):
        for g in range(groups):
            pl.when(met[g])(functools.partial(signal, semaphore, (there, g)))

    def tell_before(semaphore):
        tell(semaphore, before, with_before)

    def tell_after(semaphore):
        tell(semaphore, after, with_after)

    pl.when(first_tile)(lambda: tell_before(barrier))
    pl.when(~last_tile)(lambda: tell_after(barrier))
    for peer in peers:
        signal(barrier, (tile, peer))

    def load(source, target, at):
        copy = pltpu.make_async_copy(source, target, load_sem.at[at])
        copy.start()
        return copy

    def drain(ref, semaphore):
        pltpu.make_async_copy(ref, ref, semaphore).wait()

    inner = slice(rim, columns - rim)
    lead, tail = slice(0, rim), slice(columns - rim, columns)
    load_index = load(index_hbm, index, 0)
    load_lead = load(field_hbm.at[:, lead], field.at[:, lead], 1)
    load_tail = load(field_hbm.at[:, tail], field.at[:, tail], 2)
    load_owner = load(owner_hbm, owner, 3)
    load_interp = load(interp_hbm, interp, 4)
    load_inner = load(field_hbm.at[:, inner], field.at[:, inner], 5)
    load_shift = load(shift_hbm, shift, 6)
    load_blocks = load(blocks_hbm, blocks, 7)

    def piece(chunk):
        return slice(chunk * height, (chunk + 1) * height)

    def send(source, target, arrival, place):
        pltpu.make_async_remote_copy(
            src_ref=source, dst_ref=target, send_sem=send_sem.at[0], recv_sem=arrival,
            device_id=place, device_id_type=MESH,
        ).start()

    def exchange(kind, chunk, in_ref, recv):
        for peer in peers:
            send(cell_out.at[kind, chunk, peer], in_ref.at[chunk, me], recv.at[chunk], (tile, peer))
        in_ref[chunk, me] = cell_out[kind, chunk, me]

    def arrived(chunk, in_ref, recv):
        drain(in_ref.at[chunk, 0:last], recv.at[chunk])
        return [in_ref[chunk, g] for g in range(groups)]

    pl.semaphore_wait(
        barrier, last + jnp.where(first_tile, 0, from_before) + jnp.where(last_tile, from_after, 0)
    )
    pl.when(~first_tile)(lambda: tell_before(ready.at[1]))
    pl.when(last_tile)(lambda: tell_after(ready.at[0]))

    load_index.wait()
    left_list, right_list = index[0:1, :], index[1:2, :]
    lines = lax.broadcasted_iota(jnp.int32, (rim, rim), 0)
    left_pick = (lines == left_list).astype(jnp.float32).astype(jnp.bfloat16)
    right_pick = (lines + (columns - rim) == right_list).astype(jnp.float32).astype(jnp.bfloat16)
    load_lead.wait()
    load_tail.wait()
    for chunk in range(CHUNKS):
        part = piece(chunk)
        edge_out[chunk, 0] = mm(field[part, tail].astype(jnp.bfloat16), right_pick).astype(jnp.bfloat16)
        edge_out[chunk, 1] = mm(field[part, lead].astype(jnp.bfloat16), left_pick).astype(jnp.bfloat16)

    for chunk in range(CHUNKS):

        @pl.when(me < last)
        def _():
            send(edge_out.at[chunk, 0], edge_in.at[chunk, 0], edge_recv.at[chunk], (tile, up))

        @pl.when(me > 0)
        def _():
            send(edge_out.at[chunk, 1], edge_in.at[chunk, 1], edge_recv.at[chunk], (tile, down))

    def hand_round(cores):
        for g in cores:
            send(edge_out.at[:, 1], relay, relay_recv.at[0], (tile, g))

    pl.when((me == 0) & first_tile)(lambda: hand_round(range(1, groups, 2)))

    @pl.when((me == 0) & ~first_tile & ~last_tile)
    def _():
        relay[...] = edge_out[:, 1]
        hand_round(range(2, groups, 2))

    def send_right(source, cores):
        for part in range(FAR):
            for g in cores:
                rows_of = source.at[part * step : (part + 1) * step]
                send(rows_of, late_in.at[part, 0], late_recv.at[part, 0], (after, g))

    def late_right():
        pl.when(pre_last)(lambda: send_right(edge_out.at[:, 0], [last]))
        pl.when(~pre_last)(lambda: send_right(edge_out.at[:, 0], range(1, groups, 2)))

    @pl.when((me == last) & pre_last)
    def _():
        for g in range(1, last, 2):
            send(edge_out.at[:, 0], relay, relay_recv.at[0], (tile, g))

    pl.when((me == last) & last_tile)(late_right)

    load_owner.wait()
    owners = owner[...]
    choose = (owners == lax.broadcasted_iota(jnp.int32, (-(-groups // 8) * 8, points), 0)).astype(jnp.float32)
    order = lax.broadcasted_iota(jnp.int32, (points, points), 0) < lax.broadcasted_iota(
        jnp.int32, (points, points), 1
    )
    ranks = mm(choose.astype(jnp.bfloat16), order.astype(jnp.float32).astype(jnp.bfloat16))
    rank = jnp.sum(ranks * choose, axis=0, keepdims=True)
    slot = owners * capacity + rank.astype(jnp.int32)
    placement = (slot == lax.broadcasted_iota(jnp.int32, (slots, points), 0)).astype(jnp.float32)
    placement = placement.astype(jnp.bfloat16)
    load_interp.wait()
    ip[0:rim, :] = mm_t(interp[0:rim, :], placement).astype(jnp.bfloat16)
    ip[rim : 2 * rim, :] = mm_t(interp[extended - rim :, :], placement).astype(jnp.bfloat16)

    def spread(side, at):
        for g in range(groups):
            rim_out[g] = ip[side * rim : (side + 1) * rim, g * capacity : (g + 1) * capacity]
        rim_in[side] = rim_out[at]
        for chunk in range(CHUNKS):
            edge_in[chunk, side] = jnp.zeros((height, rim), jnp.bfloat16)

    pl.when(me == 0)(functools.partial(spread, 0, 0))
    pl.when(me == last)(functools.partial(spread, 1, last))

    @pl.when(me == 0)
    def _():
        for g in range(1, groups):
            send(rim_out.at[g], rim_in.at[0], rim_recv.at[0], (tile, g))

    @pl.when(me == last)
    def _():
        for g in range(last):
            send(rim_out.at[g], rim_in.at[1], rim_recv.at[0], (tile, g))

    ip[2 * rim :, :] = mm_t(interp[rim : extended - rim, :], placement).astype(jnp.bfloat16)
    load_inner.wait()
    base[...] = mm(field[...].astype(jnp.bfloat16), ip[2 * rim :, :])

    load_shift.wait()
    load_blocks.wait()

    def build_gram():
        for j in range(owned):
            for s in range(owned):
                total = jnp.zeros((size, size), jnp.float32)
                for c in range(bands):
                    reads = lax.rem(j + shift[j : j + 1, c : c + 1], owned) == s
                    total = total + jnp.where(reads, 1.0, 0.0) * blocks[j, c].astype(jnp.float32)
                conv[s * size : (s + 1) * size, j * size : (j + 1) * size] = total.astype(jnp.bfloat16)
        gram[...] = mm_t(conv[...], conv[...]).astype(jnp.bfloat16)

    outer = (me == 0) | (me == last)
    pl.when(~outer)(build_gram)

    @pl.when(hands_right)
    def _():
        drain(relay, relay_recv.at[0])
        pl.semaphore_wait(ready.at[1], from_after)
        send_right(relay, [me])

    for chunk in range(CHUNKS):
        pl.when(outer)(lambda: drain(edge_in.at[chunk, 0], edge_recv.at[chunk]))
        pl.when(~outer)(lambda: drain(edge_in.at[chunk], edge_recv.at[chunk]))
        edges = jnp.concatenate([edge_in[chunk, 0], edge_in[chunk, 1]], axis=1)
        subgrid = (base[piece(chunk), :] + mm(edges, ip[0 : 2 * rim, :])).astype(jnp.bfloat16)
        for g in range(groups):
            cell_out[0, chunk, g] = subgrid[:, g * capacity : (g + 1) * capacity]
        exchange(0, chunk, slot_in, slot_recv)

    @pl.when((me == last) & ~last_tile)
    def _():
        pl.semaphore_wait(ready.at[1], from_after)
        late_right()

    def late_left(source, cores):
        for part in range(FAR):
            for g in cores:
                rows_of = source.at[part * step : (part + 1) * step]
                send(rows_of, late_in.at[part, 1], late_recv.at[part, 1], (before, g))

    pl.when(last_tile & (me == 0))(lambda: late_left(edge_out.at[:, 1], range(0, groups, 2)))

    @pl.when(hands_on)
    def _():
        pl.when(me != 0)(lambda: drain(relay, relay_recv.at[0]))
        pl.when(first_tile)(lambda: pl.semaphore_wait(ready.at[0], from_before))
        late_left(relay, (me - odd, me - odd + 1))

    pl.when(outer)(build_gram)

    pl.when(outer)(lambda: drain(rim_in.at[0], rim_recv.at[0]))
    pl.when(~outer)(lambda: drain(rim_in, rim_recv.at[0]))
    for side, g in ((0, 0), (1, last)):
        product = mm_t(gram[:, g * capacity : (g + 1) * capacity], rim_in[side])
        far_gram[:, side * rim : (side + 1) * rim] = product.astype(jnp.bfloat16)

    pl.when(even & first_tile)(lambda: pl.semaphore_wait(ready.at[0], from_before))
    pl.when((me != last) & ~last_tile & ~hands_right)(lambda: pl.semaphore_wait(ready.at[1], from_after))

    def pass_on(side):
        for part in range(FAR):
            arrival = late_recv.at[part, side]
            drain(late_in.at[part, side], arrival)
            send(late_in.at[part, side], late_in.at[part, side], arrival, (tile, mate))

    pl.when(~even)(lambda: pass_on(0))
    pl.when(even & pre_last)(lambda: pass_on(1))

    for chunk in range(CHUNKS):
        far_part, row = chunk // step, chunk % step
        if row == 0:
            pl.when(even)(lambda: drain(late_in.at[far_part, 0], late_recv.at[far_part, 0]))
            pl.when(~even | ~pre_last)(lambda: drain(late_in.at[far_part, 1], late_recv.at[far_part, 1]))
        added = [mm(late_in[far_part, side, row], rim_in[side]) for side in range(2)]
        cells = arrived(chunk, slot_in, slot_recv)
        for side, g in ((0, 0), (1, last)):
            cells[g] = (cells[g].astype(jnp.float32) + added[side]).astype(jnp.bfloat16)
        gathered[chunk] = jnp.concatenate(cells, axis=1)

        def give(side):
            send(far_out.at[chunk, side], share_in.at[chunk], share_recv.at[0], (tile, mate))

        def far_shares():
            far = mm(gathered[chunk], far_gram[...])
            far_out[chunk, 1] = far[:, rim:].astype(jnp.bfloat16)

            @pl.when(last_tile)
            def _():
                send(far_out.at[chunk, 1], far_in.at[chunk, me], far_recv.at[chunk], (after, 0))

            @pl.when(even)
            def _():
                share[chunk] = far[:, :rim]
                pl.when(~last_tile)(lambda: give(1))

            @pl.when(~even)
            def _():
                share[chunk] = far[:, rim:]
                far_out[chunk, 0] = far[:, :rim].astype(jnp.bfloat16)
                give(0)

        pl.when(last_tile)(far_shares)
        adjoint = mm(gathered[chunk], gram[...]).astype(jnp.bfloat16)
        for g in range(groups):
            cell_out[1, chunk, g] = adjoint[:, g * capacity : (g + 1) * capacity]
        exchange(1, chunk, back_in, back_recv)
        pl.when(~last_tile)(far_shares)

    def add_given(side, place):
        drain(share_in, share_recv.at[0])
        far_out[:, side] = (share[...] + share_in[...].astype(jnp.float32)).astype(jnp.bfloat16)
        send(far_out.at[:, side], far_in.at[:, lax.div(me, 2)], far_recv.at[0], place)

    pl.when(even)(lambda: add_given(0, (before, last)))
    pl.when(~even & ~last_tile)(lambda: add_given(1, (after, 0)))

    for chunk in range(CHUNKS):
        back = jnp.concatenate(arrived(chunk, back_in, back_recv), axis=1)
        returned[chunk * height : (chunk + 1) * height, :] = back
        rims = mm_t(back, ip[0 : 2 * rim, :]).astype(jnp.bfloat16)
        part_out[chunk, 0] = rims[:, rim:]
        part_out[chunk, 1] = rims[:, :rim]

        @pl.when(me < last)
        def _():
            send(part_out.at[chunk, 0], part_in.at[chunk, 0], part_recv.at[chunk], (tile, up))

        @pl.when(me > 0)
        def _():
            send(part_out.at[chunk, 1], part_in.at[chunk, 1], part_recv.at[chunk], (tile, down))

        if chunk % step == step - 1:
            part = slice((chunk + 1 - step) * height, (chunk + 1) * height)
            result[part, :] = mm_t(returned[part, :], ip[2 * rim :, :])

    for chunk in range(CHUNKS):
        part = piece(chunk)
        pl.when(outer)(lambda: drain(part_in.at[chunk, 0], part_recv.at[chunk]))
        pl.when(~outer)(lambda: drain(part_in.at[chunk], part_recv.at[chunk]))

        @pl.when(me > 0)
        def _():
            result[part, lead] += mm_t(part_in[chunk, 0], left_pick)

        @pl.when(me < last)
        def _():
            result[part, tail] += mm_t(part_in[chunk, 1], right_pick)

    def add_shares(chunk, where, pick, shares):
        arrived_shares = jnp.concatenate([far_in[chunk, g] for g in range(shares)], axis=1)
        result[piece(chunk), where] += mm_t(arrived_shares, jnp.concatenate([pick] * shares, axis=1))

    def add_by_chip(where, pick):
        drain(far_in.at[:, 0:middle], far_recv.at[0])
        for chunk in range(CHUNKS):
            add_shares(chunk, where, pick, middle)

    @pl.when((me == 0) & first_tile)
    def _():
        for chunk in range(CHUNKS):
            drain(far_in.at[chunk], far_recv.at[chunk])
            add_shares(chunk, lead, left_pick, groups)

    pl.when((me == 0) & ~first_tile)(lambda: add_by_chip(lead, left_pick))
    pl.when(me == last)(lambda: add_by_chip(tail, right_pick))

    drain(cell_out.at[:, :, 0:last], send_sem.at[0])
    drain(far_out, send_sem.at[0])
    pl.when(hands_on)(lambda: drain(late_in, send_sem.at[0]))
    pl.when(hands_right)(lambda: drain(relay, send_sem.at[0]))
    pl.when((me == 0) & last_tile)(lambda: drain(far_in.at[:, 0:middle], send_sem.at[0]))
    pl.when(even & pre_last)(lambda: drain(late_in.at[:, 1], send_sem.at[0]))
    pl.when(~even)(lambda: drain(late_in.at[:, 0], send_sem.at[0]))

    pl.when((me == 0) & first_tile)(lambda: drain(far_in.at[:, 0:middle], send_sem.at[0]))
    pl.when((me == 0) & ~first_tile & ~last_tile)(lambda: drain(far_in.at[:, 0 : middle - 1], send_sem.at[0]))
    pl.when(me == last)(lambda: drain(far_in.at[:, 0 : groups // 2], send_sem.at[0]))

    @pl.when((me == 0) | (me == last))
    def _():
        drain(edge_out.at[:, 0], send_sem.at[0])
        drain(rim_out.at[0:last], send_sem.at[0])
        drain(part_out.at[:, 0], send_sem.at[0])

    @pl.when((me != 0) & (me != last))
    def _():
        drain(edge_out, send_sem.at[0])
        drain(part_out, send_sem.at[0])


def in_hbm(array):
    return pltpu.with_memory_space_constraint(array, pltpu.HBM)


def on_device(tiles, groups, field, interp, conv_blocks, band_shift, owner, edge_index):
    rows, columns = field.shape
    extended, points = interp.shape
    rim = edge_index.shape[1]
    slots = conv_blocks.shape[0] * conv_blocks.shape[2]
    capacity = slots // groups
    height = rows // CHUNKS
    half, single = jnp.bfloat16, jnp.float32
    sides = pltpu.VMEM((CHUNKS, 2, height, rim), half)
    strip = pltpu.VMEM((CHUNKS, height, rim), half)
    cells = pltpu.VMEM((CHUNKS, groups, height, capacity), half)
    dma = pltpu.SemaphoreType.DMA
    anywhere = pl.BlockSpec(memory_space=pltpu.HBM)
    return pl.pallas_call(
        functools.partial(kernel, tiles, groups, rim),
        out_shape=jax.ShapeDtypeStruct(field.shape, single),
        in_specs=[anywhere] * 6,
        out_specs=pl.BlockSpec(memory_space=pltpu.VMEM),
        scratch_shapes=[
            pltpu.VMEM(field.shape, single),
            pltpu.VMEM(interp.shape, half),
            pltpu.VMEM(conv_blocks.shape, half),
            pltpu.VMEM((1, points), jnp.int32),
            pltpu.VMEM(edge_index.shape, jnp.int32),
            pltpu.VMEM(band_shift.shape, jnp.int32),
            pltpu.VMEM((extended, slots), half),
            pltpu.VMEM((slots, slots), half),
            pltpu.VMEM((slots, slots), half),
            pltpu.VMEM((rows, slots), single),
            pltpu.VMEM((rows, slots), half),
            sides, sides, strip, pltpu.VMEM((FAR, 2, CHUNKS // FAR, height, rim), half),
            pltpu.VMEM((groups, rim, capacity), half),
            pltpu.VMEM((2, rim, capacity), half),
            pltpu.VMEM((2, CHUNKS, groups, height, capacity), half),
            cells, cells,
            pltpu.VMEM((CHUNKS, height, slots), half),
            pltpu.VMEM((slots, 2 * rim), half),
            pltpu.VMEM((CHUNKS, height, rim), single),
            strip,
            sides,
            pltpu.VMEM((CHUNKS, groups, height, rim), half),
            sides, sides,
            pltpu.SemaphoreType.REGULAR((2,)), dma((8,)), dma((1,)), dma((CHUNKS,)), dma((1,)), dma((FAR, 2)),
            dma((1,)), dma((CHUNKS,)), dma((CHUNKS,)), dma((1,)), dma((CHUNKS,)), dma((CHUNKS,)),
        ],
        compiler_params=pltpu.CompilerParams(collective_id=0, has_side_effects=True, vmem_limit_bytes=53 * 2**20),
    )(field, interp, conv_blocks, *[in_hbm(small) for small in (owner.reshape(1, -1), edge_index, band_shift)])


def solution(mesh):
    return jax.shard_map(
        functools.partial(on_device, mesh.shape["tile"], mesh.shape["conv"]),
        mesh=mesh,
        in_specs=(
            P(None, ("tile", "conv")),
            P(("tile", "conv"), None),
            P(("tile", "conv"), None, None, None),
            P(("tile", "conv"), None),
            P(("tile", "conv"), None),
            P(("tile", "conv"), None),
        ),
        out_specs=P(None, ("tile", "conv")),
        check_vma=False,
    )
```

```python
import functools

import jax
import jax.numpy as jnp
from jax import lax
from jax.experimental import pallas as pl
from jax.experimental.pallas import tpu as pltpu
from jax.sharding import PartitionSpec as P

MESH = pl.DeviceIdType.MESH
CHUNKS = 2
FAR = 2


def mm(left, right):
    return lax.dot_general(left, right, (((1,), (0,)), ((), ())), preferred_element_type=jnp.float32)


def mm_t(left, right):
    return lax.dot_general(left, right, (((1,), (1,)), ((), ())), preferred_element_type=jnp.float32)


def kernel(
    tiles, groups, rim, field_hbm, interp_hbm, blocks_hbm, owner_hbm, index_hbm, shift_hbm, result,
    field, interp, blocks, owner, index, shift, ip, conv, gram, base, returned,
    edge_out, edge_in, relay, late_in, rim_out, rim_in, cell_out, slot_in, back_in, gathered, far_gram, share, share_in, far_out, far_in, part_out, part_in,
    ready, load_sem, send_sem, edge_recv, relay_recv, late_recv, rim_recv, slot_recv, back_recv, share_recv, part_recv, far_recv,
):
    rows, columns = field.shape
    extended, points = interp.shape
    owned, bands, size = blocks.shape[0], blocks.shape[1], blocks.shape[2]
    slots = owned * size
    capacity = slots // groups
    height = rows // CHUNKS
    step = CHUNKS // FAR
    last = groups - 1
    tile, me = lax.axis_index("tile"), lax.axis_index("conv")
    after, before = lax.rem(tile + 1, tiles), lax.rem(tile + tiles - 1, tiles)
    up, down = lax.rem(me + 1, groups), lax.rem(me + last, groups)
    middle = groups // 2
    low = me < middle
    peers = [jnp.where(low, middle + k, middle - 1 - k) for k in range(middle)]
    peers += [lax.rem(me + k, middle) + jnp.where(low, 0, middle) for k in range(1, middle)]

    barrier = pltpu.get_barrier_semaphore()
    first_tile, last_tile = tile == 0, tile == tiles - 1
    odd = lax.rem(me, 2)
    even = odd == 0
    mate = me + 1 - 2 * odd
    pre_last = (tile == tiles - 2) & ~first_tile
    hands_right = pre_last & ~even & (me != last)
    hands_on = (first_tile & ~even) | (~first_tile & ~last_tile & even)

    def meet(lower, upper):
        return (upper == 0) | (lower == last) | (lax.div(lower, 2) == lax.div(upper, 2))

    with_before = [meet(g, me) for g in range(groups)]
    with_after = [meet(me, g) for g in range(groups)]
    from_before = sum(jnp.where(met, 1, 0) for met in with_before)
    from_after = sum(jnp.where(met, 1, 0) for met in with_after)

    def signal(semaphore, target):
        pl.semaphore_signal(semaphore, inc=1, device_id=target, device_id_type=MESH)

    def tell(semaphore, there, met):
        for g in range(groups):
            pl.when(met[g])(functools.partial(signal, semaphore, (there, g)))

    def tell_before(semaphore):
        tell(semaphore, before, with_before)

    def tell_after(semaphore):
        tell(semaphore, after, with_after)

    pl.when(first_tile)(lambda: tell_before(barrier))
    pl.when(~last_tile)(lambda: tell_after(barrier))
    for peer in peers:
        signal(barrier, (tile, peer))

    def load(source, target, at):
        copy = pltpu.make_async_copy(source, target, load_sem.at[at])
        copy.start()
        return copy

    def drain(ref, semaphore):
        pltpu.make_async_copy(ref, ref, semaphore).wait()

    inner = slice(rim, columns - rim)
    lead, tail = slice(0, rim), slice(columns - rim, columns)
    load_index = load(index_hbm, index, 0)
    load_lead = load(field_hbm.at[:, lead], field.at[:, lead], 0)
    load_tail = load(field_hbm.at[:, tail], field.at[:, tail], 0)
    load_owner = load(owner_hbm, owner, 1)
    load_interp = load(interp_hbm, interp, 1)
    load_inner = load(field_hbm.at[:, inner], field.at[:, inner], 2)
    load_shift = load(shift_hbm, shift, 3)
    load_blocks = load(blocks_hbm, blocks, 3)

    def piece(chunk):
        return slice(chunk * height, (chunk + 1) * height)

    def send(source, target, arrival, place):
        pltpu.make_async_remote_copy(
            src_ref=source, dst_ref=target, send_sem=send_sem.at[0], recv_sem=arrival,
            device_id=place, device_id_type=MESH,
        ).start()

    def exchange(kind, chunk, in_ref, recv):
        for peer in peers:
            send(cell_out.at[kind, chunk, peer], in_ref.at[chunk, me], recv.at[chunk], (tile, peer))
        in_ref[chunk, me] = cell_out[kind, chunk, me]

    def arrived(chunk, in_ref, recv):
        drain(in_ref.at[chunk, 0:last], recv.at[chunk])
        return [in_ref[chunk, g] for g in range(groups)]

    pl.semaphore_wait(
        barrier, last + jnp.where(first_tile, 0, from_before) + jnp.where(last_tile, from_after, 0)
    )
    pl.when(~first_tile)(lambda: tell_before(ready.at[1]))
    pl.when(last_tile)(lambda: tell_after(ready.at[0]))

    load_index.wait()
    load_lead.wait()
    load_tail.wait()
    left_list, right_list = index[0:1, :], index[1:2, :]
    lines = lax.broadcasted_iota(jnp.int32, (rim, rim), 0)
    left_pick = (lines == left_list).astype(jnp.float32).astype(jnp.bfloat16)
    right_pick = (lines + (columns - rim) == right_list).astype(jnp.float32).astype(jnp.bfloat16)
    for chunk in range(CHUNKS):
        part = piece(chunk)
        edge_out[chunk, 0] = mm(field[part, tail].astype(jnp.bfloat16), right_pick).astype(jnp.bfloat16)
        edge_out[chunk, 1] = mm(field[part, lead].astype(jnp.bfloat16), left_pick).astype(jnp.bfloat16)

    for chunk in range(CHUNKS):

        @pl.when(me < last)
        def _():
            send(edge_out.at[chunk, 0], edge_in.at[chunk, 0], edge_recv.at[chunk], (tile, up))

        @pl.when(me > 0)
        def _():
            send(edge_out.at[chunk, 1], edge_in.at[chunk, 1], edge_recv.at[chunk], (tile, down))

    def hand_round(cores):
        for g in cores:
            send(edge_out.at[:, 1], relay, relay_recv.at[0], (tile, g))

    pl.when((me == 0) & first_tile)(lambda: hand_round(range(1, groups, 2)))

    @pl.when((me == 0) & ~first_tile & ~last_tile)
    def _():
        relay[...] = edge_out[:, 1]
        hand_round(range(2, groups, 2))

    def send_right(source, cores):
        for part in range(FAR):
            for g in cores:
                rows_of = source.at[part * step : (part + 1) * step]
                send(rows_of, late_in.at[part, 0], late_recv.at[part, 0], (after, g))

    def late_right():
        pl.when(pre_last)(lambda: send_right(edge_out.at[:, 0], [last]))
        pl.when(~pre_last)(lambda: send_right(edge_out.at[:, 0], range(1, groups, 2)))

    @pl.when((me == last) & pre_last)
    def _():
        for g in range(1, last, 2):
            send(edge_out.at[:, 0], relay, relay_recv.at[0], (tile, g))

    pl.when((me == last) & last_tile)(late_right)

    load_owner.wait()
    load_interp.wait()
    owners = owner[...]
    choose = (owners == lax.broadcasted_iota(jnp.int32, (-(-groups // 8) * 8, points), 0)).astype(jnp.float32)
    order = lax.broadcasted_iota(jnp.int32, (points, points), 0) < lax.broadcasted_iota(
        jnp.int32, (points, points), 1
    )
    ranks = mm(choose.astype(jnp.bfloat16), order.astype(jnp.float32).astype(jnp.bfloat16))
    rank = jnp.sum(ranks * choose, axis=0, keepdims=True)
    slot = owners * capacity + rank.astype(jnp.int32)
    placement = (slot == lax.broadcasted_iota(jnp.int32, (slots, points), 0)).astype(jnp.float32)
    placement = placement.astype(jnp.bfloat16)
    ip[0:rim, :] = mm_t(interp[0:rim, :], placement).astype(jnp.bfloat16)
    ip[rim : 2 * rim, :] = mm_t(interp[extended - rim :, :], placement).astype(jnp.bfloat16)

    def spread(side, at):
        for g in range(groups):
            rim_out[g] = ip[side * rim : (side + 1) * rim, g * capacity : (g + 1) * capacity]
        rim_in[side] = rim_out[at]
        for chunk in range(CHUNKS):
            edge_in[chunk, side] = jnp.zeros((height, rim), jnp.bfloat16)

    pl.when(me == 0)(functools.partial(spread, 0, 0))
    pl.when(me == last)(functools.partial(spread, 1, last))

    @pl.when(me == 0)
    def _():
        for g in range(1, groups):
            send(rim_out.at[g], rim_in.at[0], rim_recv.at[0], (tile, g))

    @pl.when(me == last)
    def _():
        for g in range(last):
            send(rim_out.at[g], rim_in.at[1], rim_recv.at[0], (tile, g))

    ip[2 * rim :, :] = mm_t(interp[rim : extended - rim, :], placement).astype(jnp.bfloat16)
    load_inner.wait()
    base[...] = mm(field[...].astype(jnp.bfloat16), ip[2 * rim :, :])

    load_shift.wait()
    load_blocks.wait()

    def build_gram():
        for j in range(owned):
            for s in range(owned):
                total = jnp.zeros((size, size), jnp.float32)
                for c in range(bands):
                    reads = lax.rem(j + shift[j : j + 1, c : c + 1], owned) == s
                    total = total + jnp.where(reads, 1.0, 0.0) * blocks[j, c].astype(jnp.float32)
                conv[s * size : (s + 1) * size, j * size : (j + 1) * size] = total.astype(jnp.bfloat16)
        gram[...] = mm_t(conv[...], conv[...]).astype(jnp.bfloat16)

    outer = (me == 0) | (me == last)
    pl.when(~outer)(build_gram)

    @pl.when(hands_right)
    def _():
        drain(relay, relay_recv.at[0])
        pl.semaphore_wait(ready.at[1], from_after)
        send_right(relay, [me])

    for chunk in range(CHUNKS):
        pl.when(outer)(lambda: drain(edge_in.at[chunk, 0], edge_recv.at[chunk]))
        pl.when(~outer)(lambda: drain(edge_in.at[chunk], edge_recv.at[chunk]))
        edges = jnp.concatenate([edge_in[chunk, 0], edge_in[chunk, 1]], axis=1)
        subgrid = (base[piece(chunk), :] + mm(edges, ip[0 : 2 * rim, :])).astype(jnp.bfloat16)
        for g in range(groups):
            cell_out[0, chunk, g] = subgrid[:, g * capacity : (g + 1) * capacity]
        exchange(0, chunk, slot_in, slot_recv)

    @pl.when((me == last) & ~last_tile)
    def _():
        pl.semaphore_wait(ready.at[1], from_after)
        late_right()

    def late_left(source, cores):
        for part in range(FAR):
            for g in cores:
                rows_of = source.at[part * step : (part + 1) * step]
                send(rows_of, late_in.at[part, 1], late_recv.at[part, 1], (before, g))

    pl.when(last_tile & (me == 0))(lambda: late_left(edge_out.at[:, 1], range(0, groups, 2)))

    @pl.when(hands_on)
    def _():
        pl.when(me != 0)(lambda: drain(relay, relay_recv.at[0]))
        pl.when(first_tile)(lambda: pl.semaphore_wait(ready.at[0], from_before))
        late_left(relay, (me - odd, me - odd + 1))

    pl.when(outer)(build_gram)

    pl.when(outer)(lambda: drain(rim_in.at[0], rim_recv.at[0]))
    pl.when(~outer)(lambda: drain(rim_in, rim_recv.at[0]))
    for side, g in ((0, 0), (1, last)):
        product = mm_t(gram[:, g * capacity : (g + 1) * capacity], rim_in[side])
        far_gram[:, side * rim : (side + 1) * rim] = product.astype(jnp.bfloat16)

    pl.when(even & first_tile)(lambda: pl.semaphore_wait(ready.at[0], from_before))
    pl.when((me != last) & ~last_tile & ~hands_right)(lambda: pl.semaphore_wait(ready.at[1], from_after))

    def pass_on(side):
        for part in range(FAR):
            arrival = late_recv.at[part, side]
            drain(late_in.at[part, side], arrival)
            send(late_in.at[part, side], late_in.at[part, side], arrival, (tile, mate))

    pl.when(~even)(lambda: pass_on(0))
    pl.when(even & pre_last)(lambda: pass_on(1))

    for chunk in range(CHUNKS):
        far_part, row = chunk // step, chunk % step
        if row == 0:
            pl.when(even)(lambda: drain(late_in.at[far_part, 0], late_recv.at[far_part, 0]))
            pl.when(~even | ~pre_last)(lambda: drain(late_in.at[far_part, 1], late_recv.at[far_part, 1]))
        added = [mm(late_in[far_part, side, row], rim_in[side]) for side in range(2)]
        cells = arrived(chunk, slot_in, slot_recv)
        for side, g in ((0, 0), (1, last)):
            cells[g] = (cells[g].astype(jnp.float32) + added[side]).astype(jnp.bfloat16)
        gathered[chunk] = jnp.concatenate(cells, axis=1)

        def give(side):
            send(far_out.at[chunk, side], share_in.at[chunk], share_recv.at[0], (tile, mate))

        def far_shares():
            far = mm(gathered[chunk], far_gram[...])
            far_out[chunk, 1] = far[:, rim:].astype(jnp.bfloat16)

            @pl.when(last_tile)
            def _():
                send(far_out.at[chunk, 1], far_in.at[chunk, me], far_recv.at[chunk], (after, 0))

            @pl.when(even)
            def _():
                share[chunk] = far[:, :rim]
                pl.when(~last_tile)(lambda: give(1))

            @pl.when(~even)
            def _():
                share[chunk] = far[:, rim:]
                far_out[chunk, 0] = far[:, :rim].astype(jnp.bfloat16)
                give(0)

        pl.when(last_tile)(far_shares)
        adjoint = mm(gathered[chunk], gram[...]).astype(jnp.bfloat16)
        for g in range(groups):
            cell_out[1, chunk, g] = adjoint[:, g * capacity : (g + 1) * capacity]
        exchange(1, chunk, back_in, back_recv)
        pl.when(~last_tile)(far_shares)

    def add_given(side, place):
        drain(share_in, share_recv.at[0])
        far_out[:, side] = (share[...] + share_in[...].astype(jnp.float32)).astype(jnp.bfloat16)
        send(far_out.at[:, side], far_in.at[:, lax.div(me, 2)], far_recv.at[0], place)

    pl.when(even)(lambda: add_given(0, (before, last)))
    pl.when(~even & ~last_tile)(lambda: add_given(1, (after, 0)))

    for chunk in range(CHUNKS):
        back = jnp.concatenate(arrived(chunk, back_in, back_recv), axis=1)
        returned[chunk * height : (chunk + 1) * height, :] = back
        rims = mm_t(back, ip[0 : 2 * rim, :]).astype(jnp.bfloat16)
        part_out[chunk, 0] = rims[:, rim:]
        part_out[chunk, 1] = rims[:, :rim]

        @pl.when(me < last)
        def _():
            send(part_out.at[chunk, 0], part_in.at[chunk, 0], part_recv.at[chunk, 0], (tile, up))

        @pl.when(me > 0)
        def _():
            send(part_out.at[chunk, 1], part_in.at[chunk, 1], part_recv.at[chunk, 1], (tile, down))

        if chunk % step == step - 1:
            part = slice((chunk + 1 - step) * height, (chunk + 1) * height)
            result[part, :] = mm_t(returned[part, :], ip[2 * rim :, :])

    def add_rims(side, where, pick):
        for chunk in range(CHUNKS):
            drain(part_in.at[chunk, side], part_recv.at[chunk, side])
            result[piece(chunk), where] += mm_t(part_in[chunk, side], pick)

    pl.when(even)(lambda: add_rims(1, tail, right_pick))
    pl.when(~even)(lambda: add_rims(0, lead, left_pick))
    pl.when(even & (me != 0))(lambda: add_rims(0, lead, left_pick))
    pl.when(~even & (me != last))(lambda: add_rims(1, tail, right_pick))

    def add_shares(chunk, where, pick, shares):
        arrived_shares = jnp.concatenate([far_in[chunk, g] for g in range(shares)], axis=1)
        result[piece(chunk), where] += mm_t(arrived_shares, jnp.concatenate([pick] * shares, axis=1))

    def add_by_chip(where, pick):
        drain(far_in.at[:, 0:middle], far_recv.at[0])
        for chunk in range(CHUNKS):
            add_shares(chunk, where, pick, middle)

    @pl.when((me == 0) & first_tile)
    def _():
        for chunk in range(CHUNKS):
            drain(far_in.at[chunk], far_recv.at[chunk])
            add_shares(chunk, lead, left_pick, groups)

    pl.when((me == 0) & ~first_tile)(lambda: add_by_chip(lead, left_pick))
    pl.when(me == last)(lambda: add_by_chip(tail, right_pick))

    drain(cell_out.at[:, :, 0:last], send_sem.at[0])
    drain(far_out, send_sem.at[0])
    pl.when(hands_on)(lambda: drain(late_in, send_sem.at[0]))
    pl.when(hands_right)(lambda: drain(relay, send_sem.at[0]))
    pl.when((me == 0) & last_tile)(lambda: drain(far_in.at[:, 0:middle], send_sem.at[0]))
    pl.when(even & pre_last)(lambda: drain(late_in.at[:, 1], send_sem.at[0]))
    pl.when(~even)(lambda: drain(late_in.at[:, 0], send_sem.at[0]))

    pl.when((me == 0) & first_tile)(lambda: drain(far_in.at[:, 0:middle], send_sem.at[0]))
    pl.when((me == 0) & ~first_tile & ~last_tile)(lambda: drain(far_in.at[:, 0 : middle - 1], send_sem.at[0]))
    pl.when(me == last)(lambda: drain(far_in.at[:, 0 : groups // 2], send_sem.at[0]))

    @pl.when((me == 0) | (me == last))
    def _():
        drain(edge_out.at[:, 0], send_sem.at[0])
        drain(rim_out.at[0:last], send_sem.at[0])
        drain(part_out.at[:, 0], send_sem.at[0])

    @pl.when((me != 0) & (me != last))
    def _():
        drain(edge_out, send_sem.at[0])
        drain(part_out, send_sem.at[0])


def in_hbm(array):
    return pltpu.with_memory_space_constraint(array, pltpu.HBM)


def on_device(tiles, groups, field, interp, conv_blocks, band_shift, owner, edge_index):
    rows, columns = field.shape
    extended, points = interp.shape
    rim = edge_index.shape[1]
    slots = conv_blocks.shape[0] * conv_blocks.shape[2]
    capacity = slots // groups
    height = rows // CHUNKS
    half, single = jnp.bfloat16, jnp.float32
    sides = pltpu.VMEM((CHUNKS, 2, height, rim), half)
    strip = pltpu.VMEM((CHUNKS, height, rim), half)
    cells = pltpu.VMEM((CHUNKS, groups, height, capacity), half)
    dma = pltpu.SemaphoreType.DMA
    anywhere = pl.BlockSpec(memory_space=pltpu.HBM)
    return pl.pallas_call(
        functools.partial(kernel, tiles, groups, rim),
        out_shape=jax.ShapeDtypeStruct(field.shape, single),
        in_specs=[anywhere] * 6,
        out_specs=pl.BlockSpec(memory_space=pltpu.VMEM),
        scratch_shapes=[
            pltpu.VMEM(field.shape, single),
            pltpu.VMEM(interp.shape, half),
            pltpu.VMEM(conv_blocks.shape, half),
            pltpu.VMEM((1, points), jnp.int32),
            pltpu.VMEM(edge_index.shape, jnp.int32),
            pltpu.VMEM(band_shift.shape, jnp.int32),
            pltpu.VMEM((extended, slots), half),
            pltpu.VMEM((slots, slots), half),
            pltpu.VMEM((slots, slots), half),
            pltpu.VMEM((rows, slots), single),
            pltpu.VMEM((rows, slots), half),
            sides, sides, strip, pltpu.VMEM((FAR, 2, CHUNKS // FAR, height, rim), half),
            pltpu.VMEM((groups, rim, capacity), half),
            pltpu.VMEM((2, rim, capacity), half),
            pltpu.VMEM((2, CHUNKS, groups, height, capacity), half),
            cells, cells,
            pltpu.VMEM((CHUNKS, height, slots), half),
            pltpu.VMEM((slots, 2 * rim), half),
            pltpu.VMEM((CHUNKS, height, rim), single),
            strip,
            sides,
            pltpu.VMEM((CHUNKS, groups, height, rim), half),
            sides, sides,
            pltpu.SemaphoreType.REGULAR((2,)), dma((4,)), dma((1,)), dma((CHUNKS,)), dma((1,)), dma((FAR, 2)),
            dma((1,)), dma((CHUNKS,)), dma((CHUNKS,)), dma((1,)), dma((CHUNKS, 2)), dma((CHUNKS,)),
        ],
        compiler_params=pltpu.CompilerParams(collective_id=0, has_side_effects=True, vmem_limit_bytes=53 * 2**20),
    )(field, interp, conv_blocks, *[in_hbm(small) for small in (owner.reshape(1, -1), edge_index, band_shift)])


def solution(mesh):
    return jax.shard_map(
        functools.partial(on_device, mesh.shape["tile"], mesh.shape["conv"]),
        mesh=mesh,
        in_specs=(
            P(None, ("tile", "conv")),
            P(("tile", "conv"), None),
            P(("tile", "conv"), None, None, None),
            P(("tile", "conv"), None),
            P(("tile", "conv"), None),
            P(("tile", "conv"), None),
        ),
        out_specs=P(None, ("tile", "conv")),
        check_vma=False,
    )
```

```python
import functools

import jax
import jax.numpy as jnp
from jax import lax
from jax.experimental import pallas as pl
from jax.experimental.pallas import tpu as pltpu
from jax.sharding import PartitionSpec as P

MESH = pl.DeviceIdType.MESH
CHUNKS = 2
FAR = 2


def mm(left, right):
    return lax.dot_general(left, right, (((1,), (0,)), ((), ())), preferred_element_type=jnp.float32)


def mm_t(left, right):
    return lax.dot_general(left, right, (((1,), (1,)), ((), ())), preferred_element_type=jnp.float32)


def kernel(
    tiles, groups, rim, field_hbm, interp_hbm, blocks_hbm, owner_hbm, index_hbm, shift_hbm, result,
    field, interp, blocks, owner, index, shift, ip, conv, gram, base, returned,
    edge_out, edge_in, relay, late_in, rim_out, rim_in, cell_out, slot_in, back_in, gathered, far_gram, share, share_in, far_out, far_in, part_out, part_in,
    ready, load_sem, send_sem, edge_recv, relay_recv, late_recv, rim_recv, slot_recv, back_recv, share_recv, part_recv, far_recv,
):
    rows, columns = field.shape
    extended, points = interp.shape
    owned, bands, size = blocks.shape[0], blocks.shape[1], blocks.shape[2]
    slots = owned * size
    capacity = slots // groups
    height = rows // CHUNKS
    step = CHUNKS // FAR
    last = groups - 1
    tile, me = lax.axis_index("tile"), lax.axis_index("conv")
    after, before = lax.rem(tile + 1, tiles), lax.rem(tile + tiles - 1, tiles)
    up, down = lax.rem(me + 1, groups), lax.rem(me + last, groups)
    middle = groups // 2
    low = me < middle
    peers = [jnp.where(low, middle + k, middle - 1 - k) for k in range(middle)]
    peers += [lax.rem(me + k, middle) + jnp.where(low, 0, middle) for k in range(1, middle)]

    barrier = pltpu.get_barrier_semaphore()
    first_tile, last_tile = tile == 0, tile == tiles - 1
    odd = lax.rem(me, 2)
    even = odd == 0
    mate = me + 1 - 2 * odd
    pre_last = (tile == tiles - 2) & ~first_tile
    hands_right = pre_last & ~even & (me != last)
    hands_on = (first_tile & ~even) | (~first_tile & ~last_tile & even)

    def meet(lower, upper):
        return (upper == 0) | (lower == last) | (lax.div(lower, 2) == lax.div(upper, 2))

    with_before = [meet(g, me) for g in range(groups)]
    with_after = [meet(me, g) for g in range(groups)]
    from_before = sum(jnp.where(met, 1, 0) for met in with_before)
    from_after = sum(jnp.where(met, 1, 0) for met in with_after)

    def signal(semaphore, target):
        pl.semaphore_signal(semaphore, inc=1, device_id=target, device_id_type=MESH)

    def tell(semaphore, there, met):
        for g in range(groups):
            pl.when(met[g])(functools.partial(signal, semaphore, (there, g)))

    def tell_before(semaphore):
        tell(semaphore, before, with_before)

    def tell_after(semaphore):
        tell(semaphore, after, with_after)

    pl.when(first_tile)(lambda: tell_before(barrier))
    pl.when(~last_tile)(lambda: tell_after(barrier))
    for peer in peers:
        signal(barrier, (tile, peer))

    def load(source, target, at):
        copy = pltpu.make_async_copy(source, target, load_sem.at[at])
        copy.start()
        return copy

    def drain(ref, semaphore):
        pltpu.make_async_copy(ref, ref, semaphore).wait()

    inner = slice(rim, columns - rim)
    lead, tail = slice(0, rim), slice(columns - rim, columns)
    load_index = load(index_hbm, index, 0)
    load_lead = load(field_hbm.at[:, lead], field.at[:, lead], 0)
    load_tail = load(field_hbm.at[:, tail], field.at[:, tail], 0)
    load_owner = load(owner_hbm, owner, 1)
    load_interp = load(interp_hbm, interp, 1)
    load_inner = load(field_hbm.at[:, inner], field.at[:, inner], 2)
    load_shift = load(shift_hbm, shift, 3)
    load_blocks = load(blocks_hbm, blocks, 3)

    def piece(chunk):
        return slice(chunk * height, (chunk + 1) * height)

    def send(source, target, arrival, place):
        pltpu.make_async_remote_copy(
            src_ref=source, dst_ref=target, send_sem=send_sem.at[0], recv_sem=arrival,
            device_id=place, device_id_type=MESH,
        ).start()

    def exchange(kind, chunk, in_ref, recv):
        for peer in peers:
            send(cell_out.at[kind, chunk, peer], in_ref.at[chunk, me], recv.at[chunk], (tile, peer))
        in_ref[chunk, me] = cell_out[kind, chunk, me]

    def arrived(chunk, in_ref, recv):
        drain(in_ref.at[chunk, 0:last], recv.at[chunk])
        return [in_ref[chunk, g] for g in range(groups)]

    pl.semaphore_wait(
        barrier, last + jnp.where(first_tile, 0, from_before) + jnp.where(last_tile, from_after, 0)
    )
    pl.when(~first_tile)(lambda: tell_before(ready.at[1]))
    pl.when(last_tile)(lambda: tell_after(ready.at[0]))

    load_index.wait()
    load_lead.wait()
    load_tail.wait()
    left_list, right_list = index[0:1, :], index[1:2, :]
    lines = lax.broadcasted_iota(jnp.int32, (rim, rim), 0)
    left_pick = (lines == left_list).astype(jnp.float32).astype(jnp.bfloat16)
    right_pick = (lines + (columns - rim) == right_list).astype(jnp.float32).astype(jnp.bfloat16)
    for chunk in range(CHUNKS):
        part = piece(chunk)
        edge_out[chunk, 0] = mm(field[part, tail].astype(jnp.bfloat16), right_pick).astype(jnp.bfloat16)
        edge_out[chunk, 1] = mm(field[part, lead].astype(jnp.bfloat16), left_pick).astype(jnp.bfloat16)

    for chunk in range(CHUNKS):

        @pl.when(me < last)
        def _():
            send(edge_out.at[chunk, 0], edge_in.at[chunk, 0], edge_recv.at[chunk], (tile, up))

        @pl.when(me > 0)
        def _():
            send(edge_out.at[chunk, 1], edge_in.at[chunk, 1], edge_recv.at[chunk], (tile, down))

    def hand_round(cores):
        for g in cores:
            send(edge_out.at[:, 1], relay, relay_recv.at[0], (tile, g))

    pl.when((me == 0) & first_tile)(lambda: hand_round(range(1, groups, 2)))

    @pl.when((me == 0) & ~first_tile & ~last_tile)
    def _():
        relay[...] = edge_out[:, 1]
        hand_round(range(2, groups, 2))

    def send_right(source, cores):
        for part in range(FAR):
            for g in cores:
                rows_of = source.at[part * step : (part + 1) * step]
                send(rows_of, late_in.at[part, 0], late_recv.at[part, 0], (after, g))

    def late_right():
        pl.when(pre_last)(lambda: send_right(edge_out.at[:, 0], [last]))
        pl.when(~pre_last)(lambda: send_right(edge_out.at[:, 0], range(1, groups, 2)))

    @pl.when((me == last) & pre_last)
    def _():
        for g in range(1, last, 2):
            send(edge_out.at[:, 0], relay, relay_recv.at[0], (tile, g))

    pl.when((me == last) & last_tile)(late_right)

    load_owner.wait()
    load_interp.wait()
    owners = owner[...]
    choose = (owners == lax.broadcasted_iota(jnp.int32, (-(-groups // 8) * 8, points), 0)).astype(jnp.float32)
    order = lax.broadcasted_iota(jnp.int32, (points, points), 0) < lax.broadcasted_iota(
        jnp.int32, (points, points), 1
    )
    ranks = mm(choose.astype(jnp.bfloat16), order.astype(jnp.float32).astype(jnp.bfloat16))
    rank = jnp.sum(ranks * choose, axis=0, keepdims=True)
    slot = owners * capacity + rank.astype(jnp.int32)
    placement = (slot == lax.broadcasted_iota(jnp.int32, (slots, points), 0)).astype(jnp.float32)
    placement = placement.astype(jnp.bfloat16)
    ip[0:rim, :] = mm_t(interp[0:rim, :], placement).astype(jnp.bfloat16)
    ip[rim : 2 * rim, :] = mm_t(interp[extended - rim :, :], placement).astype(jnp.bfloat16)

    def spread(side, at):
        for g in range(groups):
            rim_out[g] = ip[side * rim : (side + 1) * rim, g * capacity : (g + 1) * capacity]
        rim_in[side] = rim_out[at]
        for chunk in range(CHUNKS):
            edge_in[chunk, side] = jnp.zeros((height, rim), jnp.bfloat16)

    pl.when(me == 0)(functools.partial(spread, 0, 0))
    pl.when(me == last)(functools.partial(spread, 1, last))

    @pl.when(me == 0)
    def _():
        for g in range(1, groups):
            send(rim_out.at[g], rim_in.at[0], rim_recv.at[0], (tile, g))

    @pl.when(me == last)
    def _():
        for g in range(last):
            send(rim_out.at[g], rim_in.at[1], rim_recv.at[0], (tile, g))

    ip[2 * rim :, :] = mm_t(interp[rim : extended - rim, :], placement).astype(jnp.bfloat16)
    load_inner.wait()
    base[...] = mm(field[...].astype(jnp.bfloat16), ip[2 * rim :, :])

    load_shift.wait()
    load_blocks.wait()

    def build_gram():
        for j in range(owned):
            for s in range(owned):
                total = jnp.zeros((size, size), jnp.float32)
                for c in range(bands):
                    reads = lax.rem(j + shift[j : j + 1, c : c + 1], owned) == s
                    total = total + jnp.where(reads, 1.0, 0.0) * blocks[j, c].astype(jnp.float32)
                conv[s * size : (s + 1) * size, j * size : (j + 1) * size] = total.astype(jnp.bfloat16)
        gram[...] = mm_t(conv[...], conv[...]).astype(jnp.bfloat16)

    outer = (me == 0) | (me == last)
    pl.when(~outer)(build_gram)

    @pl.when(hands_right)
    def _():
        drain(relay, relay_recv.at[0])
        pl.semaphore_wait(ready.at[1], from_after)
        send_right(relay, [me])

    for chunk in range(CHUNKS):
        pl.when(outer)(lambda: drain(edge_in.at[chunk, 0], edge_recv.at[chunk]))
        pl.when(~outer)(lambda: drain(edge_in.at[chunk], edge_recv.at[chunk]))
        edges = jnp.concatenate([edge_in[chunk, 0], edge_in[chunk, 1]], axis=1)
        subgrid = (base[piece(chunk), :] + mm(edges, ip[0 : 2 * rim, :])).astype(jnp.bfloat16)
        for g in range(groups):
            cell_out[0, chunk, g] = subgrid[:, g * capacity : (g + 1) * capacity]
        exchange(0, chunk, slot_in, slot_recv)

    @pl.when((me == last) & ~last_tile)
    def _():
        pl.semaphore_wait(ready.at[1], from_after)
        late_right()

    def late_left(source, cores):
        for part in range(FAR):
            for g in cores:
                rows_of = source.at[part * step : (part + 1) * step]
                send(rows_of, late_in.at[part, 1], late_recv.at[part, 1], (before, g))

    pl.when(last_tile & (me == 0))(lambda: late_left(edge_out.at[:, 1], range(0, groups, 2)))

    @pl.when(hands_on)
    def _():
        pl.when(me != 0)(lambda: drain(relay, relay_recv.at[0]))
        pl.when(first_tile)(lambda: pl.semaphore_wait(ready.at[0], from_before))
        late_left(relay, (me - odd, me - odd + 1))

    pl.when(outer)(build_gram)

    pl.when(outer)(lambda: drain(rim_in.at[0], rim_recv.at[0]))
    pl.when(~outer)(lambda: drain(rim_in, rim_recv.at[0]))
    for side, g in ((0, 0), (1, last)):
        product = mm_t(gram[:, g * capacity : (g + 1) * capacity], rim_in[side])
        far_gram[:, side * rim : (side + 1) * rim] = product.astype(jnp.bfloat16)

    pl.when(even & first_tile)(lambda: pl.semaphore_wait(ready.at[0], from_before))
    pl.when((me != last) & ~last_tile & ~hands_right)(lambda: pl.semaphore_wait(ready.at[1], from_after))

    def pass_on(side):
        for part in range(FAR):
            arrival = late_recv.at[part, side]
            drain(late_in.at[part, side], arrival)
            send(late_in.at[part, side], late_in.at[part, side], arrival, (tile, mate))

    pl.when(~even)(lambda: pass_on(0))
    pl.when(even & pre_last)(lambda: pass_on(1))

    for chunk in range(CHUNKS):
        far_part, row = chunk // step, chunk % step
        if row == 0:
            pl.when(even)(lambda: drain(late_in.at[far_part, 0], late_recv.at[far_part, 0]))
            pl.when(~even | ~pre_last)(lambda: drain(late_in.at[far_part, 1], late_recv.at[far_part, 1]))
        added = [mm(late_in[far_part, side, row], rim_in[side]) for side in range(2)]
        cells = arrived(chunk, slot_in, slot_recv)
        for side, g in ((0, 0), (1, last)):
            cells[g] = (cells[g].astype(jnp.float32) + added[side]).astype(jnp.bfloat16)
        gathered[chunk] = jnp.concatenate(cells, axis=1)

        def give(side):
            send(far_out.at[chunk, side], share_in.at[chunk], share_recv.at[0], (tile, mate))

        def last_share():
            product = mm(gathered[chunk], far_gram[:, rim:])
            far_out[chunk, 1] = product.astype(jnp.bfloat16)
            return product

        def first_share():
            return mm(gathered[chunk], far_gram[:, :rim])

        def give_first(kept):
            far_out[chunk, 0] = kept.astype(jnp.bfloat16)
            give(0)

        @pl.when(last_tile)
        def _():
            last_share()
            send(far_out.at[chunk, 1], far_in.at[chunk, me], far_recv.at[chunk], (after, 0))

        adjoint = mm(gathered[chunk], gram[...]).astype(jnp.bfloat16)
        for g in range(groups):
            cell_out[1, chunk, g] = adjoint[:, g * capacity : (g + 1) * capacity]
        exchange(1, chunk, back_in, back_recv)

        @pl.when(even)
        def _():
            share[chunk] = first_share()

        pl.when(~even)(lambda: give_first(first_share()))

        @pl.when(~last_tile)
        def _():
            kept = last_share()

            @pl.when(~even)
            def _():
                share[chunk] = kept

            pl.when(even)(lambda: give(1))

    def add_given(side, place):
        drain(share_in, share_recv.at[0])
        far_out[:, side] = (share[...] + share_in[...].astype(jnp.float32)).astype(jnp.bfloat16)
        send(far_out.at[:, side], far_in.at[:, lax.div(me, 2)], far_recv.at[0], place)

    pl.when(even)(lambda: add_given(0, (before, last)))
    pl.when(~even & ~last_tile)(lambda: add_given(1, (after, 0)))

    for chunk in range(CHUNKS):
        back = jnp.concatenate(arrived(chunk, back_in, back_recv), axis=1)
        returned[chunk * height : (chunk + 1) * height, :] = back
        rims = mm_t(back, ip[0 : 2 * rim, :]).astype(jnp.bfloat16)
        part_out[chunk, 0] = rims[:, rim:]
        part_out[chunk, 1] = rims[:, :rim]

        @pl.when(me < last)
        def _():
            send(part_out.at[chunk, 0], part_in.at[chunk, 0], part_recv.at[chunk, 0], (tile, up))

        @pl.when(me > 0)
        def _():
            send(part_out.at[chunk, 1], part_in.at[chunk, 1], part_recv.at[chunk, 1], (tile, down))

        if chunk % step == step - 1:
            part = slice((chunk + 1 - step) * height, (chunk + 1) * height)
            result[part, :] = mm_t(returned[part, :], ip[2 * rim :, :])

    def add_rims(side, where, pick):
        for chunk in range(CHUNKS):
            drain(part_in.at[chunk, side], part_recv.at[chunk, side])
            result[piece(chunk), where] += mm_t(part_in[chunk, side], pick)

    pl.when(even)(lambda: add_rims(1, tail, right_pick))
    pl.when(~even)(lambda: add_rims(0, lead, left_pick))
    pl.when(even & (me != 0))(lambda: add_rims(0, lead, left_pick))
    pl.when(~even & (me != last))(lambda: add_rims(1, tail, right_pick))

    def add_shares(chunk, where, pick, shares):
        arrived_shares = jnp.concatenate([far_in[chunk, g] for g in range(shares)], axis=1)
        result[piece(chunk), where] += mm_t(arrived_shares, jnp.concatenate([pick] * shares, axis=1))

    def add_by_chip(where, pick):
        drain(far_in.at[:, 0:middle], far_recv.at[0])
        for chunk in range(CHUNKS):
            add_shares(chunk, where, pick, middle)

    @pl.when((me == 0) & first_tile)
    def _():
        for chunk in range(CHUNKS):
            drain(far_in.at[chunk], far_recv.at[chunk])
            add_shares(chunk, lead, left_pick, groups)

    pl.when((me == 0) & ~first_tile)(lambda: add_by_chip(lead, left_pick))
    pl.when(me == last)(lambda: add_by_chip(tail, right_pick))

    drain(cell_out.at[:, :, 0:last], send_sem.at[0])
    drain(far_out, send_sem.at[0])
    pl.when(hands_on)(lambda: drain(late_in, send_sem.at[0]))
    pl.when(hands_right)(lambda: drain(relay, send_sem.at[0]))
    pl.when((me == 0) & last_tile)(lambda: drain(far_in.at[:, 0:middle], send_sem.at[0]))
    pl.when(even & pre_last)(lambda: drain(late_in.at[:, 1], send_sem.at[0]))
    pl.when(~even)(lambda: drain(late_in.at[:, 0], send_sem.at[0]))

    pl.when((me == 0) & first_tile)(lambda: drain(far_in.at[:, 0:middle], send_sem.at[0]))
    pl.when((me == 0) & ~first_tile & ~last_tile)(lambda: drain(far_in.at[:, 0 : middle - 1], send_sem.at[0]))
    pl.when(me == last)(lambda: drain(far_in.at[:, 0 : groups // 2], send_sem.at[0]))

    @pl.when((me == 0) | (me == last))
    def _():
        drain(edge_out.at[:, 0], send_sem.at[0])
        drain(rim_out.at[0:last], send_sem.at[0])
        drain(part_out.at[:, 0], send_sem.at[0])

    @pl.when((me != 0) & (me != last))
    def _():
        drain(edge_out, send_sem.at[0])
        drain(part_out, send_sem.at[0])


def in_hbm(array):
    return pltpu.with_memory_space_constraint(array, pltpu.HBM)


def on_device(tiles, groups, field, interp, conv_blocks, band_shift, owner, edge_index):
    rows, columns = field.shape
    extended, points = interp.shape
    rim = edge_index.shape[1]
    slots = conv_blocks.shape[0] * conv_blocks.shape[2]
    capacity = slots // groups
    height = rows // CHUNKS
    half, single = jnp.bfloat16, jnp.float32
    sides = pltpu.VMEM((CHUNKS, 2, height, rim), half)
    strip = pltpu.VMEM((CHUNKS, height, rim), half)
    cells = pltpu.VMEM((CHUNKS, groups, height, capacity), half)
    dma = pltpu.SemaphoreType.DMA
    anywhere = pl.BlockSpec(memory_space=pltpu.HBM)
    return pl.pallas_call(
        functools.partial(kernel, tiles, groups, rim),
        out_shape=jax.ShapeDtypeStruct(field.shape, single),
        in_specs=[anywhere] * 6,
        out_specs=pl.BlockSpec(memory_space=pltpu.VMEM),
        scratch_shapes=[
            pltpu.VMEM(field.shape, single),
            pltpu.VMEM(interp.shape, half),
            pltpu.VMEM(conv_blocks.shape, half),
            pltpu.VMEM((1, points), jnp.int32),
            pltpu.VMEM(edge_index.shape, jnp.int32),
            pltpu.VMEM(band_shift.shape, jnp.int32),
            pltpu.VMEM((extended, slots), half),
            pltpu.VMEM((slots, slots), half),
            pltpu.VMEM((slots, slots), half),
            pltpu.VMEM((rows, slots), single),
            pltpu.VMEM((rows, slots), half),
            sides, sides, strip, pltpu.VMEM((FAR, 2, CHUNKS // FAR, height, rim), half),
            pltpu.VMEM((groups, rim, capacity), half),
            pltpu.VMEM((2, rim, capacity), half),
            pltpu.VMEM((2, CHUNKS, groups, height, capacity), half),
            cells, cells,
            pltpu.VMEM((CHUNKS, height, slots), half),
            pltpu.VMEM((slots, 2 * rim), half),
            pltpu.VMEM((CHUNKS, height, rim), single),
            strip,
            sides,
            pltpu.VMEM((CHUNKS, groups, height, rim), half),
            sides, sides,
            pltpu.SemaphoreType.REGULAR((2,)), dma((4,)), dma((1,)), dma((CHUNKS,)), dma((1,)), dma((FAR, 2)),
            dma((1,)), dma((CHUNKS,)), dma((CHUNKS,)), dma((1,)), dma((CHUNKS, 2)), dma((CHUNKS,)),
        ],
        compiler_params=pltpu.CompilerParams(collective_id=0, has_side_effects=True, vmem_limit_bytes=53 * 2**20),
    )(field, interp, conv_blocks, *[in_hbm(small) for small in (owner.reshape(1, -1), edge_index, band_shift)])


def solution(mesh):
    return jax.shard_map(
        functools.partial(on_device, mesh.shape["tile"], mesh.shape["conv"]),
        mesh=mesh,
        in_specs=(
            P(None, ("tile", "conv")),
            P(("tile", "conv"), None),
            P(("tile", "conv"), None, None, None),
            P(("tile", "conv"), None),
            P(("tile", "conv"), None),
            P(("tile", "conv"), None),
        ),
        out_specs=P(None, ("tile", "conv")),
        check_vma=False,
    )
```

```python
import functools

import jax
import jax.numpy as jnp
from jax import lax
from jax.experimental import pallas as pl
from jax.experimental.pallas import tpu as pltpu
from jax.sharding import PartitionSpec as P

MESH = pl.DeviceIdType.MESH
CHUNKS = 2
FAR = 2


def mm(left, right):
    return lax.dot_general(left, right, (((1,), (0,)), ((), ())), preferred_element_type=jnp.float32)


def mm_t(left, right):
    return lax.dot_general(left, right, (((1,), (1,)), ((), ())), preferred_element_type=jnp.float32)


def kernel(
    tiles, groups, rim, field_hbm, interp_hbm, blocks_hbm, owner_hbm, index_hbm, shift_hbm, result,
    field, interp, blocks, owner, index, shift, ip, conv, gram, base, returned,
    edge_out, edge_in, relay, late_in, rim_out, rim_in, cell_out, slot_in, back_in, gathered, far_gram, share, share_in, far_out, far_in, part_out, part_in,
    ready, load_sem, send_sem, edge_recv, relay_recv, late_recv, rim_recv, slot_recv, back_recv, share_recv, part_recv, far_recv,
):
    rows, columns = field.shape
    extended, points = interp.shape
    owned, bands, size = blocks.shape[0], blocks.shape[1], blocks.shape[2]
    slots = owned * size
    capacity = slots // groups
    height = rows // CHUNKS
    step = CHUNKS // FAR
    last = groups - 1
    tile, me = lax.axis_index("tile"), lax.axis_index("conv")
    after, before = lax.rem(tile + 1, tiles), lax.rem(tile + tiles - 1, tiles)
    up, down = lax.rem(me + 1, groups), lax.rem(me + last, groups)
    middle = groups // 2
    low = me < middle
    peers = [jnp.where(low, middle + k, middle - 1 - k) for k in range(middle)]
    peers += [lax.rem(me + k, middle) + jnp.where(low, 0, middle) for k in range(1, middle)]

    barrier = pltpu.get_barrier_semaphore()
    first_tile, last_tile = tile == 0, tile == tiles - 1
    odd = lax.rem(me, 2)
    even = odd == 0
    mate = me + 1 - 2 * odd
    pre_last = (tile == tiles - 2) & ~first_tile
    hands_right = pre_last & ~even & (me != last)
    hands_on = (first_tile & ~even) | (~first_tile & ~last_tile & even)

    def meet(lower, upper):
        return (upper == 0) | (lower == last) | (lax.div(lower, 2) == lax.div(upper, 2))

    with_before = [meet(g, me) for g in range(groups)]
    with_after = [meet(me, g) for g in range(groups)]
    from_before = sum(jnp.where(met, 1, 0) for met in with_before)
    from_after = sum(jnp.where(met, 1, 0) for met in with_after)

    def signal(semaphore, target):
        pl.semaphore_signal(semaphore, inc=1, device_id=target, device_id_type=MESH)

    def tell(semaphore, there, met):
        for g in range(groups):
            pl.when(met[g])(functools.partial(signal, semaphore, (there, g)))

    def tell_before(semaphore):
        tell(semaphore, before, with_before)

    def tell_after(semaphore):
        tell(semaphore, after, with_after)

    def load(source, target, at):
        copy = pltpu.make_async_copy(source, target, load_sem.at[at])
        copy.start()
        return copy

    def drain(ref, semaphore):
        pltpu.make_async_copy(ref, ref, semaphore).wait()

    inner = slice(rim, columns - rim)
    lead, tail = slice(0, rim), slice(columns - rim, columns)
    load_lead = load(field_hbm.at[:, lead], field.at[:, lead], 0)
    load_tail = load(field_hbm.at[:, tail], field.at[:, tail], 0)
    load_index = load(index_hbm, index, 0)

    pl.when(first_tile)(lambda: tell_before(barrier))
    pl.when(~last_tile)(lambda: tell_after(barrier))
    for peer in peers:
        signal(barrier, (tile, peer))

    load_owner = load(owner_hbm, owner, 1)
    load_interp = load(interp_hbm, interp, 1)
    load_inner = load(field_hbm.at[:, inner], field.at[:, inner], 2)
    load_shift = load(shift_hbm, shift, 3)
    load_blocks = load(blocks_hbm, blocks, 3)

    def piece(chunk):
        return slice(chunk * height, (chunk + 1) * height)

    def send(source, target, arrival, place):
        pltpu.make_async_remote_copy(
            src_ref=source, dst_ref=target, send_sem=send_sem.at[0], recv_sem=arrival,
            device_id=place, device_id_type=MESH,
        ).start()

    def exchange(kind, chunk, in_ref, recv):
        for peer in peers:
            send(cell_out.at[kind, chunk, peer], in_ref.at[chunk, me], recv.at[chunk], (tile, peer))
        in_ref[chunk, me] = cell_out[kind, chunk, me]

    def arrived(chunk, in_ref, recv):
        drain(in_ref.at[chunk, 0:last], recv.at[chunk])
        return [in_ref[chunk, g] for g in range(groups)]

    pl.semaphore_wait(
        barrier, last + jnp.where(first_tile, 0, from_before) + jnp.where(last_tile, from_after, 0)
    )
    pl.when(~first_tile)(lambda: tell_before(ready.at[1]))
    pl.when(last_tile)(lambda: tell_after(ready.at[0]))

    load_index.wait()
    load_lead.wait()
    load_tail.wait()
    left_list, right_list = index[0:1, :], index[1:2, :]
    lines = lax.broadcasted_iota(jnp.int32, (rim, rim), 0)
    left_pick = (lines == left_list).astype(jnp.float32).astype(jnp.bfloat16)
    right_pick = (lines + (columns - rim) == right_list).astype(jnp.float32).astype(jnp.bfloat16)
    for chunk in range(CHUNKS):
        part = piece(chunk)
        edge_out[chunk, 0] = mm(field[part, tail].astype(jnp.bfloat16), right_pick).astype(jnp.bfloat16)
        edge_out[chunk, 1] = mm(field[part, lead].astype(jnp.bfloat16), left_pick).astype(jnp.bfloat16)

    for chunk in range(CHUNKS):

        @pl.when(me < last)
        def _():
            send(edge_out.at[chunk, 0], edge_in.at[chunk, 0], edge_recv.at[chunk], (tile, up))

        @pl.when(me > 0)
        def _():
            send(edge_out.at[chunk, 1], edge_in.at[chunk, 1], edge_recv.at[chunk], (tile, down))

    def hand_round(cores):
        for g in cores:
            send(edge_out.at[:, 1], relay, relay_recv.at[0], (tile, g))

    pl.when((me == 0) & first_tile)(lambda: hand_round(range(1, groups, 2)))

    @pl.when((me == 0) & ~first_tile & ~last_tile)
    def _():
        relay[...] = edge_out[:, 1]
        hand_round(range(2, groups, 2))

    def send_right(source, cores):
        for part in range(FAR):
            for g in cores:
                rows_of = source.at[part * step : (part + 1) * step]
                send(rows_of, late_in.at[part, 0], late_recv.at[part, 0], (after, g))

    def late_right():
        pl.when(pre_last)(lambda: send_right(edge_out.at[:, 0], [last]))
        pl.when(~pre_last)(lambda: send_right(edge_out.at[:, 0], range(1, groups, 2)))

    @pl.when((me == last) & pre_last)
    def _():
        for g in range(1, last, 2):
            send(edge_out.at[:, 0], relay, relay_recv.at[0], (tile, g))

    pl.when((me == last) & last_tile)(late_right)

    load_owner.wait()
    load_interp.wait()
    owners = owner[...]
    choose = (owners == lax.broadcasted_iota(jnp.int32, (-(-groups // 8) * 8, points), 0)).astype(jnp.float32)
    order = lax.broadcasted_iota(jnp.int32, (points, points), 0) < lax.broadcasted_iota(
        jnp.int32, (points, points), 1
    )
    ranks = mm(choose.astype(jnp.bfloat16), order.astype(jnp.float32).astype(jnp.bfloat16))
    rank = jnp.sum(ranks * choose, axis=0, keepdims=True)
    slot = owners * capacity + rank.astype(jnp.int32)
    placement = (slot == lax.broadcasted_iota(jnp.int32, (slots, points), 0)).astype(jnp.float32)
    placement = placement.astype(jnp.bfloat16)
    ip[0:rim, :] = mm_t(interp[0:rim, :], placement).astype(jnp.bfloat16)
    ip[rim : 2 * rim, :] = mm_t(interp[extended - rim :, :], placement).astype(jnp.bfloat16)

    def spread(side, at):
        for g in range(groups):
            rim_out[g] = ip[side * rim : (side + 1) * rim, g * capacity : (g + 1) * capacity]
        rim_in[side] = rim_out[at]
        for chunk in range(CHUNKS):
            edge_in[chunk, side] = jnp.zeros((height, rim), jnp.bfloat16)

    pl.when(me == 0)(functools.partial(spread, 0, 0))
    pl.when(me == last)(functools.partial(spread, 1, last))

    @pl.when(me == 0)
    def _():
        for g in range(1, groups):
            send(rim_out.at[g], rim_in.at[0], rim_recv.at[0], (tile, g))

    @pl.when(me == last)
    def _():
        for g in range(last):
            send(rim_out.at[g], rim_in.at[1], rim_recv.at[0], (tile, g))

    ip[2 * rim :, :] = mm_t(interp[rim : extended - rim, :], placement).astype(jnp.bfloat16)
    load_inner.wait()
    base[...] = mm(field[...].astype(jnp.bfloat16), ip[2 * rim :, :])

    load_shift.wait()
    load_blocks.wait()

    def build_gram():
        for j in range(owned):
            for s in range(owned):
                total = jnp.zeros((size, size), jnp.float32)
                for c in range(bands):
                    reads = lax.rem(j + shift[j : j + 1, c : c + 1], owned) == s
                    total = total + jnp.where(reads, 1.0, 0.0) * blocks[j, c].astype(jnp.float32)
                conv[s * size : (s + 1) * size, j * size : (j + 1) * size] = total.astype(jnp.bfloat16)
        gram[...] = mm_t(conv[...], conv[...]).astype(jnp.bfloat16)

    outer = (me == 0) | (me == last)
    pl.when(~outer)(build_gram)

    @pl.when(hands_right)
    def _():
        drain(relay, relay_recv.at[0])
        pl.semaphore_wait(ready.at[1], from_after)
        send_right(relay, [me])

    for chunk in range(CHUNKS):
        pl.when(outer)(lambda: drain(edge_in.at[chunk, 0], edge_recv.at[chunk]))
        pl.when(~outer)(lambda: drain(edge_in.at[chunk], edge_recv.at[chunk]))
        edges = jnp.concatenate([edge_in[chunk, 0], edge_in[chunk, 1]], axis=1)
        subgrid = (base[piece(chunk), :] + mm(edges, ip[0 : 2 * rim, :])).astype(jnp.bfloat16)
        for g in range(groups):
            cell_out[0, chunk, g] = subgrid[:, g * capacity : (g + 1) * capacity]
        exchange(0, chunk, slot_in, slot_recv)

    @pl.when((me == last) & ~last_tile)
    def _():
        pl.semaphore_wait(ready.at[1], from_after)
        late_right()

    def late_left(source, cores):
        for part in range(FAR):
            for g in cores:
                rows_of = source.at[part * step : (part + 1) * step]
                send(rows_of, late_in.at[part, 1], late_recv.at[part, 1], (before, g))

    pl.when(last_tile & (me == 0))(lambda: late_left(edge_out.at[:, 1], range(0, groups, 2)))

    @pl.when(hands_on)
    def _():
        pl.when(me != 0)(lambda: drain(relay, relay_recv.at[0]))
        pl.when(first_tile)(lambda: pl.semaphore_wait(ready.at[0], from_before))
        late_left(relay, (me - odd, me - odd + 1))

    pl.when(outer)(build_gram)

    pl.when(outer)(lambda: drain(rim_in.at[0], rim_recv.at[0]))
    pl.when(~outer)(lambda: drain(rim_in, rim_recv.at[0]))
    for side, g in ((0, 0), (1, last)):
        product = mm_t(gram[:, g * capacity : (g + 1) * capacity], rim_in[side])
        far_gram[:, side * rim : (side + 1) * rim] = product.astype(jnp.bfloat16)

    pl.when(even & first_tile)(lambda: pl.semaphore_wait(ready.at[0], from_before))
    pl.when((me != last) & ~last_tile & ~hands_right)(lambda: pl.semaphore_wait(ready.at[1], from_after))

    def pass_on(side):
        for part in range(FAR):
            arrival = late_recv.at[part, side]
            drain(late_in.at[part, side], arrival)
            send(late_in.at[part, side], late_in.at[part, side], arrival, (tile, mate))

    pl.when(~even)(lambda: pass_on(0))
    pl.when(even & pre_last)(lambda: pass_on(1))

    for chunk in range(CHUNKS):
        far_part, row = chunk // step, chunk % step
        if row == 0:
            pl.when(even)(lambda: drain(late_in.at[far_part, 0], late_recv.at[far_part, 0]))
            pl.when(~even | ~pre_last)(lambda: drain(late_in.at[far_part, 1], late_recv.at[far_part, 1]))
        added = [mm(late_in[far_part, side, row], rim_in[side]) for side in range(2)]
        cells = arrived(chunk, slot_in, slot_recv)
        for side, g in ((0, 0), (1, last)):
            cells[g] = (cells[g].astype(jnp.float32) + added[side]).astype(jnp.bfloat16)
        gathered[chunk] = jnp.concatenate(cells, axis=1)

        def give(side):
            send(far_out.at[chunk, side], share_in.at[chunk], share_recv.at[0], (tile, mate))

        def last_share():
            product = mm(gathered[chunk], far_gram[:, rim:])
            far_out[chunk, 1] = product.astype(jnp.bfloat16)
            return product

        def first_share():
            return mm(gathered[chunk], far_gram[:, :rim])

        def give_first(kept):
            far_out[chunk, 0] = kept.astype(jnp.bfloat16)
            give(0)

        @pl.when(last_tile)
        def _():
            last_share()
            send(far_out.at[chunk, 1], far_in.at[chunk, me], far_recv.at[chunk], (after, 0))

        adjoint = mm(gathered[chunk], gram[...]).astype(jnp.bfloat16)
        for g in range(groups):
            cell_out[1, chunk, g] = adjoint[:, g * capacity : (g + 1) * capacity]
        exchange(1, chunk, back_in, back_recv)

        @pl.when(even)
        def _():
            share[chunk] = first_share()

        pl.when(~even)(lambda: give_first(first_share()))

        @pl.when(~last_tile)
        def _():
            kept = last_share()

            @pl.when(~even)
            def _():
                share[chunk] = kept

            pl.when(even)(lambda: give(1))

    def add_given(side, place):
        drain(share_in, share_recv.at[0])
        far_out[:, side] = (share[...] + share_in[...].astype(jnp.float32)).astype(jnp.bfloat16)
        send(far_out.at[:, side], far_in.at[:, lax.div(me, 2)], far_recv.at[0], place)

    pl.when(even)(lambda: add_given(0, (before, last)))
    pl.when(~even & ~last_tile)(lambda: add_given(1, (after, 0)))

    for chunk in range(CHUNKS):
        back = jnp.concatenate(arrived(chunk, back_in, back_recv), axis=1)
        returned[chunk * height : (chunk + 1) * height, :] = back
        rims = mm_t(back, ip[0 : 2 * rim, :]).astype(jnp.bfloat16)
        part_out[chunk, 0] = rims[:, rim:]
        part_out[chunk, 1] = rims[:, :rim]

        @pl.when(me < last)
        def _():
            send(part_out.at[chunk, 0], part_in.at[chunk, 0], part_recv.at[chunk, 0], (tile, up))

        @pl.when(me > 0)
        def _():
            send(part_out.at[chunk, 1], part_in.at[chunk, 1], part_recv.at[chunk, 1], (tile, down))

        if chunk % step == step - 1:
            part = slice((chunk + 1 - step) * height, (chunk + 1) * height)
            result[part, :] = mm_t(returned[part, :], ip[2 * rim :, :])

    def add_rims(side, where, pick):
        for chunk in range(CHUNKS):
            drain(part_in.at[chunk, side], part_recv.at[chunk, side])
            result[piece(chunk), where] += mm_t(part_in[chunk, side], pick)

    pl.when(even)(lambda: add_rims(1, tail, right_pick))
    pl.when(~even)(lambda: add_rims(0, lead, left_pick))
    pl.when(even & (me != 0))(lambda: add_rims(0, lead, left_pick))
    pl.when(~even & (me != last))(lambda: add_rims(1, tail, right_pick))

    def add_shares(chunk, where, pick, shares):
        arrived_shares = jnp.concatenate([far_in[chunk, g] for g in range(shares)], axis=1)
        result[piece(chunk), where] += mm_t(arrived_shares, jnp.concatenate([pick] * shares, axis=1))

    def add_by_chip(where, pick):
        drain(far_in.at[:, 0:middle], far_recv.at[0])
        for chunk in range(CHUNKS):
            add_shares(chunk, where, pick, middle)

    @pl.when((me == 0) & first_tile)
    def _():
        for chunk in range(CHUNKS):
            drain(far_in.at[chunk], far_recv.at[chunk])
            add_shares(chunk, lead, left_pick, groups)

    pl.when((me == 0) & ~first_tile)(lambda: add_by_chip(lead, left_pick))
    pl.when(me == last)(lambda: add_by_chip(tail, right_pick))

    drain(cell_out.at[:, :, 0:last], send_sem.at[0])
    drain(far_out, send_sem.at[0])
    pl.when(hands_on)(lambda: drain(late_in, send_sem.at[0]))
    pl.when(hands_right)(lambda: drain(relay, send_sem.at[0]))
    pl.when((me == 0) & last_tile)(lambda: drain(far_in.at[:, 0:middle], send_sem.at[0]))
    pl.when(even & pre_last)(lambda: drain(late_in.at[:, 1], send_sem.at[0]))
    pl.when(~even)(lambda: drain(late_in.at[:, 0], send_sem.at[0]))

    pl.when((me == 0) & first_tile)(lambda: drain(far_in.at[:, 0:middle], send_sem.at[0]))
    pl.when((me == 0) & ~first_tile & ~last_tile)(lambda: drain(far_in.at[:, 0 : middle - 1], send_sem.at[0]))
    pl.when(me == last)(lambda: drain(far_in.at[:, 0 : groups // 2], send_sem.at[0]))

    @pl.when((me == 0) | (me == last))
    def _():
        drain(edge_out.at[:, 0], send_sem.at[0])
        drain(rim_out.at[0:last], send_sem.at[0])
        drain(part_out.at[:, 0], send_sem.at[0])

    @pl.when((me != 0) & (me != last))
    def _():
        drain(edge_out, send_sem.at[0])
        drain(part_out, send_sem.at[0])


def in_hbm(array):
    return pltpu.with_memory_space_constraint(array, pltpu.HBM)


def on_device(tiles, groups, field, interp, conv_blocks, band_shift, owner, edge_index):
    rows, columns = field.shape
    extended, points = interp.shape
    rim = edge_index.shape[1]
    slots = conv_blocks.shape[0] * conv_blocks.shape[2]
    capacity = slots // groups
    height = rows // CHUNKS
    half, single = jnp.bfloat16, jnp.float32
    sides = pltpu.VMEM((CHUNKS, 2, height, rim), half)
    strip = pltpu.VMEM((CHUNKS, height, rim), half)
    cells = pltpu.VMEM((CHUNKS, groups, height, capacity), half)
    dma = pltpu.SemaphoreType.DMA
    anywhere = pl.BlockSpec(memory_space=pltpu.HBM)
    return pl.pallas_call(
        functools.partial(kernel, tiles, groups, rim),
        out_shape=jax.ShapeDtypeStruct(field.shape, single),
        in_specs=[anywhere] * 6,
        out_specs=pl.BlockSpec(memory_space=pltpu.VMEM),
        scratch_shapes=[
            pltpu.VMEM(field.shape, single),
            pltpu.VMEM(interp.shape, half),
            pltpu.VMEM(conv_blocks.shape, half),
            pltpu.VMEM((1, points), jnp.int32),
            pltpu.VMEM(edge_index.shape, jnp.int32),
            pltpu.VMEM(band_shift.shape, jnp.int32),
            pltpu.VMEM((extended, slots), half),
            pltpu.VMEM((slots, slots), half),
            pltpu.VMEM((slots, slots), half),
            pltpu.VMEM((rows, slots), single),
            pltpu.VMEM((rows, slots), half),
            sides, sides, strip, pltpu.VMEM((FAR, 2, CHUNKS // FAR, height, rim), half),
            pltpu.VMEM((groups, rim, capacity), half),
            pltpu.VMEM((2, rim, capacity), half),
            pltpu.VMEM((2, CHUNKS, groups, height, capacity), half),
            cells, cells,
            pltpu.VMEM((CHUNKS, height, slots), half),
            pltpu.VMEM((slots, 2 * rim), half),
            pltpu.VMEM((CHUNKS, height, rim), single),
            strip,
            sides,
            pltpu.VMEM((CHUNKS, groups, height, rim), half),
            sides, sides,
            pltpu.SemaphoreType.REGULAR((2,)), dma((4,)), dma((1,)), dma((CHUNKS,)), dma((1,)), dma((FAR, 2)),
            dma((1,)), dma((CHUNKS,)), dma((CHUNKS,)), dma((1,)), dma((CHUNKS, 2)), dma((CHUNKS,)),
        ],
        compiler_params=pltpu.CompilerParams(collective_id=0, has_side_effects=True, vmem_limit_bytes=53 * 2**20),
    )(field, interp, conv_blocks, *[in_hbm(small) for small in (owner.reshape(1, -1), edge_index, band_shift)])


def solution(mesh):
    return jax.shard_map(
        functools.partial(on_device, mesh.shape["tile"], mesh.shape["conv"]),
        mesh=mesh,
        in_specs=(
            P(None, ("tile", "conv")),
            P(("tile", "conv"), None),
            P(("tile", "conv"), None, None, None),
            P(("tile", "conv"), None),
            P(("tile", "conv"), None),
            P(("tile", "conv"), None),
        ),
        out_specs=P(None, ("tile", "conv")),
        check_vma=False,
    )
```
